128 devices in a mesh: gz: 2 (over x_hi), row: 8 (over y, core), col: 8 (over z, x_lo).
Axes of the slice: x: 4 (x_hi: 2, x_lo: 2; x = x_hi * 2 + x_lo), y: 4, z: 4, core: 2. Of those that a mesh axis runs over, the one named last changes fastest.
Arguments:
- sections: bfloat16 [4, 4096, 4096], P('gz', 'row', 'col'), may hold values from -6 to 6
- priors: int32 [2, 4, 16, 16], P(None, 'gz', 'row', 'col'), may hold values from -64 to 64
- row_order: int32 [16], replicated, may hold values from 0 to 15, each once
Outputs:
- mesh_flows: float32 [16, 128], P('row')
The draws below stay inside these ranges and needn't reach their ends.
Inputs may be any that keep to these rules, and one draw needn't show every extreme that they name: A permutation of the patch rows: mesh row m holds patch row row_order[m].
All inputs are finite; a program needn't handle non-finite values.
Results may differ from the reference program's by a relative error of at most 0.0003.
Values may be sent and summed in bfloat16 or wider, within the bound.
A program may use at most 64 MiB of HBM per device.

```python
import math
import jax
import jax.numpy as jnp
from jax import lax

PATCH = 512
STRIDE = 256
LAGS = 128
MAXOFF = 64
HALO = 256
SECTIONS = 4
HEIGHT = 4096
WIDTH = 4096
GRID_R = 16
GRID_C = 16


def shared_shifts(key):
    shift_key = jax.random.fold_in(key, 4242)
    reach = MAXOFF // 8
    starts = jax.random.randint(jax.random.fold_in(shift_key, 1), (2, SECTIONS), -reach, reach + 1)
    slopes = jax.random.randint(jax.random.fold_in(shift_key, 2), (2, SECTIONS), -reach, reach + 1)
    return (starts, slopes)


def moved_by(starts, slopes, coords, extent):
    return starts[:, None] + slopes[:, None] * coords[None, :] // extent


def draw_sections(key, part):
    starts, slopes = shared_shifts(key)
    rows_all = jnp.arange(HEIGHT, dtype=jnp.int32)
    cols_all = jnp.arange(WIDTH, dtype=jnp.int32)
    row_shift = moved_by(starts[0], slopes[0], rows_all, HEIGHT)
    col_shift = moved_by(starts[1], slopes[1], cols_all, WIDTH)
    margin = MAXOFF
    texture_key = jax.random.fold_in(key, 11)
    noise_key = jax.random.fold_in(key, 12)
    texture = jax.random.normal(texture_key, (HEIGHT + 2 * margin, WIDTH + 2 * margin), jnp.float32)
    noise = jax.random.normal(noise_key, (SECTIONS, HEIGHT, WIDTH), jnp.float32)
    signal_weight = 0.9
    noise_weight = 0.45
    level = 1.0
    row_index = rows_all[None, :] - row_shift + margin
    col_index = cols_all[None, :] - col_shift + margin

    def one_section(row_pick, col_pick):
        return jnp.take(jnp.take(texture, row_pick, axis=0), col_pick, axis=1)
    moved = jax.vmap(one_section)(row_index, col_index)
    result = level * (signal_weight * moved + noise_weight * noise)
    return jnp.clip(result, -6.0, 6.0).astype(jnp.bfloat16)


def draw_priors(key, part):
    starts, slopes = shared_shifts(key)
    center_gap = PATCH // 2 - HALO // 2
    row_centers = jnp.clip(jnp.arange(GRID_R, dtype=jnp.int32) * STRIDE + center_gap, 0, HEIGHT - 1)
    col_centers = jnp.clip(jnp.arange(GRID_C, dtype=jnp.int32) * STRIDE + center_gap, 0, WIDTH - 1)
    row_shift = moved_by(starts[0], slopes[0], row_centers, HEIGHT)
    col_shift = moved_by(starts[1], slopes[1], col_centers, WIDTH)
    row_lag = jnp.roll(row_shift, -1, axis=0) - row_shift
    col_lag = jnp.roll(col_shift, -1, axis=0) - col_shift
    slack = MAXOFF // 2
    jitter = jax.random.randint(jax.random.fold_in(key, 13), (2, SECTIONS, GRID_R, GRID_C), -slack, slack + 1)
    row_prior = row_lag[:, :, None] + jitter[0]
    col_prior = col_lag[:, None, :] + jitter[1]
    result = jnp.clip(jnp.stack([row_prior, col_prior], axis=0), -MAXOFF, MAXOFF)
    result = result.at[0, 0, 0, 0].set(MAXOFF)
    result = result.at[0, SECTIONS - 1, 0, 0].set(-MAXOFF)
    result = result.at[1, 0, 0, 0].set(-MAXOFF)
    result = result.at[1, SECTIONS - 1, 0, 0].set(MAXOFF)
    return result.astype(jnp.int32)


def setup_inputs(seed: int = 0) -> dict:
    splits = jax.random.split(jax.random.key(seed), 4)
    sections = draw_sections(jax.random.fold_in(splits[3], 71), 0)
    priors = draw_priors(jax.random.fold_in(splits[3], 71), 0)
    row_order = jax.random.permutation(splits[2], GRID_R).astype(jnp.int32)
    return dict(sections=sections, priors=priors, row_order=row_order)


def dft_tables(length):
    frequencies = jnp.arange(length, dtype=jnp.int32)
    angles = jnp.mod(frequencies[:, None] * frequencies[None, :], length).astype(jnp.float32) * (2.0 * math.pi / length)
    cosine = jnp.cos(angles)
    sine_part = jnp.sin(angles)
    minus_table = jnp.concatenate([cosine, -sine_part], axis=1).astype(jnp.bfloat16)
    plus_table = jnp.concatenate([cosine, sine_part], axis=1).astype(jnp.bfloat16)
    return minus_table, plus_table


def spectra_of(patches, minus_table, plus_table):
    length = patches.shape[-1]
    row_pass = jnp.einsum('nxy,yk->nxk', patches.astype(jnp.float32), minus_table.astype(jnp.float32)).astype(jnp.bfloat16)
    real_rows = row_pass[:, :, :length]
    imag_rows = row_pass[:, :, length:]
    upper_stack = jnp.concatenate([real_rows, imag_rows], axis=1).astype(jnp.float32)
    lower_stack = jnp.concatenate([imag_rows, real_rows], axis=1).astype(jnp.float32)
    spec_real = jnp.einsum('kx,nxm->nkm', plus_table.astype(jnp.float32), upper_stack) / length
    spec_imag = jnp.einsum('kx,nxm->nkm', minus_table.astype(jnp.float32), lower_stack) / length
    return jnp.stack([spec_real, spec_imag], axis=1).astype(jnp.bfloat16)


def lag_angles(offsets, length):
    frequencies = jnp.arange(length, dtype=jnp.int32)
    shifts = offsets[:, None] + jnp.arange(LAGS, dtype=jnp.int32)[None, :] - LAGS // 2
    angles = jnp.mod(shifts[:, :, None] * frequencies[None, None, :], length).astype(jnp.float32) * (2.0 * math.pi / length)
    return jnp.cos(angles), jnp.sin(angles)


def flows_of(first_spec, second_spec, offsets):
    length = first_spec.shape[-1]
    first_real = first_spec[:, 0].astype(jnp.float32)
    first_imag = first_spec[:, 1].astype(jnp.float32)
    second_real = second_spec[:, 0].astype(jnp.float32)
    second_imag = second_spec[:, 1].astype(jnp.float32)
    prod_real = (first_real * second_real + first_imag * second_imag).astype(jnp.bfloat16)
    prod_imag = (first_real * second_imag - first_imag * second_real).astype(jnp.bfloat16)
    row_cosine, row_sine = lag_angles(offsets[0], length)
    column_cosine, column_sine = lag_angles(offsets[1], length)
    products = jnp.concatenate([prod_real, prod_imag], axis=2).astype(jnp.float32)
    column_real = jnp.concatenate([column_cosine, -column_sine], axis=2).astype(jnp.bfloat16).astype(jnp.float32)
    column_imag = jnp.concatenate([column_sine, column_cosine], axis=2).astype(jnp.bfloat16).astype(jnp.float32)
    half_real = jnp.einsum('nkl,nul->nku', products, column_real).astype(jnp.bfloat16)
    half_imag = jnp.einsum('nkl,nul->nku', products, column_imag).astype(jnp.bfloat16)
    row_table = jnp.concatenate([row_cosine, -row_sine], axis=2).astype(jnp.bfloat16).astype(jnp.float32)
    stacked = jnp.concatenate([half_real, half_imag], axis=1).astype(jnp.float32)
    surface = jnp.einsum('ntk,nku->ntu', row_table, stacked) / length
    weights = surface * surface
    displacement = (jnp.arange(LAGS, dtype=jnp.int32) - LAGS // 2).astype(jnp.float32)
    weight_sum = 1.0 + jnp.sum(weights, axis=(1, 2))
    row_shift = jnp.sum(weights * displacement[None, :, None], axis=(1, 2)) / weight_sum
    column_shift = jnp.sum(weights * displacement[None, None, :], axis=(1, 2)) / weight_sum
    return jnp.stack([offsets[0].astype(jnp.float32) + row_shift, offsets[1].astype(jnp.float32) + column_shift], axis=0)


def reference(sections, priors, row_order):
    minus_table, plus_table = dft_tables(PATCH)
    margin = HALO // 2
    padded = jnp.pad(sections, ((0, 0), (margin, HALO - margin), (margin, HALO - margin)))
    place_count = GRID_R * GRID_C
    offsets_all = jnp.transpose(priors, (2, 3, 0, 1)).reshape(place_count, 2, SECTIONS)
    positions = jnp.arange(place_count, dtype=jnp.int32)

    def one_place(inputs):
        position, offsets = inputs
        top_edge = (position // GRID_C) * STRIDE
        left_edge = (position % GRID_C) * STRIDE
        window = lax.dynamic_slice(padded, (jnp.int32(0), top_edge.astype(jnp.int32), left_edge.astype(jnp.int32)), (SECTIONS, PATCH, PATCH))
        spectra = spectra_of(window, minus_table, plus_table)
        following = jnp.concatenate([spectra[1:], spectra[:1]], axis=0)
        return flows_of(spectra, following, offsets)

    all_flows = lax.map(one_place, (positions, offsets_all))
    flow_table = jnp.transpose(all_flows.reshape(GRID_R, GRID_C, 2, SECTIONS), (2, 3, 0, 1))
    picked = flow_table[:, :, row_order, :]
    return jnp.transpose(picked, (2, 0, 1, 3)).reshape(GRID_R, 2 * SECTIONS * GRID_C)
```

```python
import functools

import jax
import jax.numpy as jnp
import ml_dtypes
import numpy as np
from jax import lax
from jax.experimental import pallas as pl
from jax.experimental.pallas import tpu as pltpu
from jax.sharding import PartitionSpec as P

PATCH = 512
LAGS = 128
UNIT = 128
MESH = pl.DeviceIdType.MESH
BF16 = jnp.bfloat16
F32 = jnp.float32


def slots():
    m = np.arange(128)
    freq = np.concatenate([2 * m, 2 * m, 2 * m + 1, 2 * m + 1])
    sine = np.concatenate([np.zeros(128), np.ones(128), np.zeros(128), np.ones(128)]).astype(bool)
    weight = np.full(512, 2.0)
    freq[128], sine[128] = 256, False
    weight[0] = weight[128] = 1.0
    return freq, sine, weight


def forward_table():
    freq, sine, _ = slots()
    angle = (freq[:, None] * np.arange(PATCH)[None, :]) % PATCH * (2.0 * np.pi / PATCH)
    return np.where(sine[:, None], np.sin(angle), np.cos(angle)).astype(ml_dtypes.bfloat16)


def lag_tables():
    freq, _, weight = slots()
    lag = np.arange(LAGS) - LAGS // 2
    angle = (freq[None, :] * lag[:, None]) % PATCH * (2.0 * np.pi / PATCH)
    return (np.cos(angle) * weight).astype(np.float32), (np.sin(angle) * weight).astype(np.float32)


def phase_rows():
    freq, sine, _ = slots()
    rows = np.zeros((8, 512), np.int32)
    rows[0] = freq
    rows[1] = np.where(sine, -128, 0)
    rows[2] = np.where(sine, 0, 128)
    rows[3] = 1
    rows[3, 128] = 0
    return rows


def cross_chunk(a, b, m_ref, kb, lb, rc):
    top = pl.multiple_of(kb * 256 + rc * 16, 16)
    low = pl.multiple_of(kb * 256 + 128 + rc * 16, 16)
    lc, ls = pl.ds(lb * 256, 128), pl.ds(lb * 256 + 128, 128)
    rt, rl = pl.ds(top, 16), pl.ds(low, 16)
    a1, a2, a3, a4 = a[rt, lc], a[rt, ls], a[rl, lc], a[rl, ls]
    b1, b2, b3, b4 = b[rt, lc], b[rt, ls], b[rl, lc], b[rl, ls]
    p33, p44 = a3 * b3, a4 * b4
    u1, u2 = a1 * b2 - a2 * b1, a3 * b4 - a4 * b3
    v1, v2 = a1 * b3 - a3 * b1, a2 * b4 - a4 * b2
    ss = (a1 * b4 + a4 * b1) - (a2 * b3 + a3 * b2)
    if kb == 0:
        k0 = lax.broadcasted_iota(jnp.int32, (16, 128), 0) + rc * 16 == 0
        z33, z44, zu2 = jnp.where(k0, 0.0, p33), jnp.where(k0, 0.0, p44), jnp.where(k0, 0.0, u2)
    else:
        z33, z44, zu2 = p33, p44, u2
    t1, t2 = a1 * b1 + z33, a2 * b2 + z44
    cc, cs, sc = t1 + t2, u1 + zu2, v1 + v2
    if kb == 0:
        sc, ss = jnp.where(k0, p33 + p44, sc), jnp.where(k0, u2, ss)
    if lb == 0:
        l0 = lax.broadcasted_iota(jnp.int32, (16, 128), 1) == 0
        cc, cs = jnp.where(l0, t1, cc), jnp.where(l0, t2, cs)
        if kb == 0:
            sc = jnp.where(l0, jnp.where(k0, p33, v1), sc)
            ss = jnp.where(l0, jnp.where(k0, p44, v2), ss)
        else:
            sc, ss = jnp.where(l0, v1, sc), jnp.where(l0, v2, ss)
    m_ref[rt, lc] = cc.astype(BF16)
    m_ref[rt, ls] = cs.astype(BF16)
    m_ref[rl, lc] = sc.astype(BF16)
    m_ref[rl, ls] = ss.astype(BF16)


def kernel(
    sections, priors, row_order, table, table_t, lag_cos, lag_sin, phases, out,
    m_buf, pg_buf, zm, zpg, a_s, b_s, mix, prior_own, prior_guest, u_s, v_s, sums, flow_send, flow_recv, grid_send, grid_recv,
    local_sem, send_x, recv_x, send_r, recv_r, send_p, recv_p, send_c, recv_c,
):
    gz, row, col = lax.axis_index("gz"), lax.axis_index("row"), lax.axis_index("col")
    n_gz, n_row, n_col = lax.axis_size("gz"), lax.axis_size("row"), lax.axis_size("col")
    x_lo = lax.rem(col, 2)
    z = lax.div(col, 2)
    has_left, has_right = z > 0, z < n_col // 2 - 1
    has_out = jnp.logical_or(jnp.logical_and(x_lo == 0, has_left), jnp.logical_and(x_lo == 1, has_right))
    has_in = jnp.logical_or(jnp.logical_and(x_lo == 1, has_left), jnp.logical_and(x_lo == 0, has_right))
    has_up, has_down = row > 0, row < n_row - 1
    side = 2 * x_lo - 1
    a_id = (gz, row, col - side)
    b_id = (1 - gz, row, col - side)
    n_id = (gz, row, col + side)
    z_out = (gz, row, col + 2 * side)
    z_in = (gz, row, col - 2 * side)
    up_id, down_id = (gz, row - 1, col), (gz, row + 1, col)

    def al(v):
        return pl.multiple_of(v, 128)

    c0 = al(128 + 512 * x_lo)
    near, outer = al(512 + 128 * x_lo), al(128 + 896 * x_lo)
    near_p, outer_p = al(512 - 384 * x_lo), al(128 + 384 * x_lo)
    c1 = al(640 - 512 * x_lo)
    near_g, outer_g = al(640 - 128 * x_lo), al(1024 - 896 * x_lo)
    m_far_out, m_far_in = al(1152 * x_lo), al(1152 - 1152 * x_lo)
    side_in, side_out = al(640 - 640 * x_lo), al(640 * x_lo)
    body = pl.ds(128, 512)
    p_buf, g_buf = pg_buf.at[0], pg_buf.at[1]

    own_m = pltpu.make_async_copy(sections.at[x_lo], m_buf.at[body, pl.ds(c0, 512)], local_sem.at[0])
    own_p = pltpu.make_async_copy(sections.at[1 - x_lo], p_buf.at[body, pl.ds(128, 512)], local_sem.at[1])
    own_m.start()
    own_p.start()

    peers_plane = [(lax.rem(gz + dg, n_gz), row, lax.rem(col + dc, n_col)) for dg in range(n_gz) for dc in range(n_col) if dg or dc]
    peers_column = [(gz, lax.rem(row + d, n_row), col) for d in range(1, n_row)]
    barrier = pltpu.get_barrier_semaphore()
    for peer in peers_plane + peers_column:
        pl.semaphore_signal(barrier, inc=1, device_id=peer, device_id_type=MESH)

    for c in range(2):
        for ii in range(2):
            for jj in range(2):
                r = c * 4 + ii * 2 + jj
                prior_own[0, r : r + 1, :] = jnp.full((1, 128), priors[c, 0, ii, jj], jnp.int32)
                prior_own[1, r : r + 1, :] = jnp.full((1, 128), priors[c, 1, ii, jj], jnp.int32)

    @pl.when(row == 0)
    def _():
        m_buf[0:128, :] = jnp.zeros((128, 1280), BF16)
        pg_buf[:, 0:128, :] = jnp.zeros((2, 128, 768), BF16)

    @pl.when(row == n_row - 1)
    def _():
        m_buf[640:768, :] = jnp.zeros((128, 1280), BF16)
        pg_buf[:, 640:768, :] = jnp.zeros((2, 128, 768), BF16)

    @pl.when(jnp.logical_not(has_left))
    def _():
        m_buf[:, 0:128] = jnp.zeros((768, 128), BF16)
        pg_buf[x_lo, :, 0:128] = jnp.zeros((768, 128), BF16)

    @pl.when(jnp.logical_not(has_right))
    def _():
        m_buf[:, 1152:1280] = jnp.zeros((768, 128), BF16)
        pg_buf[1 - x_lo, :, 640:768] = jnp.zeros((768, 128), BF16)

    own_m.wait()
    own_p.wait()
    pl.semaphore_wait(barrier, len(peers_plane) + len(peers_column))

    def remote(k, src, dst, device):
        return pltpu.make_async_remote_copy(
            src_ref=src, dst_ref=dst, send_sem=send_x.at[k], recv_sem=recv_x.at[k], device_id=device, device_id_type=MESH
        )

    def strip(ref, start, width=128):
        return ref.at[body, pl.ds(start, width)]

    pa_outer = remote(0, strip(p_buf, outer_p), strip(m_buf, outer), a_id)
    pa_near = remote(1, strip(p_buf, near_p), strip(m_buf, near), a_id)
    m_a = remote(2, strip(m_buf, near), strip(p_buf, side_out), a_id)
    m_n = remote(3, strip(m_buf, outer), strip(p_buf, side_in), n_id)
    pa_mid = remote(4, strip(p_buf, 256, 256), strip(m_buf, al(c0 + 128), 256), a_id)
    mz_own = remote(5, strip(m_buf, outer), strip(m_buf, m_far_in), z_out)
    mb_tile = remote(6, strip(m_buf, c0, 512), strip(g_buf, 128, 512), b_id)
    mz_guest = remote(7, strip(m_buf, outer_g), strip(m_buf, m_far_out), z_in)
    mb_near = remote(8, strip(m_buf, near_g), strip(g_buf, side_in), b_id)
    mb_far = remote(9, strip(m_buf, m_far_out), strip(g_buf, side_out), b_id)
    prior_id = (gz + x_lo * (1 - 2 * gz), row, col - side)
    prior_send = remote(10, prior_own.at[1], prior_guest, prior_id)

    prior_send.start()
    pa_outer.start()
    mb_tile.start()
    pl.when(has_out)(mz_own.start)
    pa_near.start()
    m_a.start()
    pl.when(has_out)(m_n.start)
    pa_mid.start()

    landed = {
        0: strip(m_buf, outer_g), 1: strip(m_buf, near_g), 2: strip(p_buf, side_in), 3: strip(p_buf, side_out),
        4: strip(m_buf, al(c1 + 128), 256), 5: strip(m_buf, m_far_in), 6: strip(g_buf, 128, 512), 7: strip(m_buf, m_far_out),
        8: strip(g_buf, side_out), 9: strip(g_buf, side_in), 10: prior_guest,
    }
    when_recv = {3: has_out, 5: has_in, 7: has_out, 9: has_in}

    def landing(k):
        ref = landed[k]
        return remote(k, ref, ref, a_id)

    def rows_of(k, ref, start, width):
        cols = pl.ds(start, width)
        up = pltpu.make_async_remote_copy(
            src_ref=ref.at[pl.ds(128, 128), cols], dst_ref=ref.at[pl.ds(640, 128), cols],
            send_sem=send_r.at[2 * k], recv_sem=recv_r.at[2 * k], device_id=up_id, device_id_type=MESH,
        )
        down = pltpu.make_async_remote_copy(
            src_ref=ref.at[pl.ds(512, 128), cols], dst_ref=ref.at[pl.ds(0, 128), cols],
            send_sem=send_r.at[2 * k + 1], recv_sem=recv_r.at[2 * k + 1], device_id=down_id, device_id_type=MESH,
        )
        return up, down

    pieces = {
        0: (m_buf, outer_g, 128), 1: (m_buf, near_g, 128), 2: (p_buf, side_in, 128), 3: (p_buf, side_out, 128),
        4: (m_buf, al(c1 + 128), 256), 5: (m_buf, m_far_in, 128), 6: (g_buf, 128, 512), 7: (m_buf, m_far_out, 128),
        8: (g_buf, side_out, 128), 9: (g_buf, side_in, 128), 10: (m_buf, c0, 512), 11: (p_buf, 128, 512),
    }

    def send_rows(k):
        up, down = rows_of(k, *pieces[k])
        pl.when(has_up)(up.start)
        pl.when(has_down)(down.start)

    def wait_rows(k):
        up, down = rows_of(k, *pieces[k])
        pl.when(has_down)(up.wait_recv)
        pl.when(has_up)(down.wait_recv)

    def wait_sent_rows(k):
        up, down = rows_of(k, *pieces[k])
        pl.when(has_up)(up.wait_send)
        pl.when(has_down)(down.wait_send)

    def guarded(k, do):
        if k in when_recv:
            pl.when(when_recv[k])(do)
        else:
            do()

    def arrive(k, forward=None, cond=None):
        def do():
            landing(k).wait_recv()
            send_rows(k)

        guarded(k, do)
        if forward is not None:
            if cond is None:
                forward.start()
            else:
                pl.when(cond)(forward.start)

    send_rows(10)
    send_rows(11)
    landing(10).wait_recv()

    freq, off_u, off_v, mask_v = phases[0:1, :], phases[1:2, :], phases[2:3, :], phases[3:4, :]
    for t in range(2):
        value = prior_own[0] if t == 0 else prior_guest[...]
        sign = (1 - 2 * x_lo) * (1 - 2 * t)
        wide = jnp.concatenate([value] * 4, axis=1) * sign
        turn = wide * freq
        scale = 2.0 * np.pi / PATCH
        u_s[8 * t : 8 * t + 8, :] = jnp.cos(((turn + off_u) & (PATCH - 1)).astype(F32) * scale)
        v_s[8 * t : 8 * t + 8, :] = (
            jnp.cos(((turn + off_v) & (PATCH - 1)).astype(F32) * scale) * mask_v.astype(F32) * sign.astype(F32)
        )

    arrive(0, mz_guest, has_in)
    arrive(5)
    arrive(1, mb_near)
    arrive(2)
    arrive(3)
    arrive(7, mb_far, has_out)
    arrive(4)
    arrive(6)
    arrive(8)
    arrive(9)
    for k in range(12):
        guarded(k, functools.partial(wait_rows, k))

    def first_pass(src, dst, block):
        at = al(block * 256)
        for i in range(2):
            dst[i, :, pl.ds(at, 256)] = jnp.dot(
                table[...], src[pl.ds(256 * i, 512), pl.ds(at, 256)], preferred_element_type=F32
            ).astype(BF16)

    pl.loop(0, 5)(lambda b: first_pass(m_buf, zm, b))
    pl.loop(0, 3)(lambda b: first_pass(p_buf, zpg.at[0], b))
    pl.loop(0, 3)(lambda b: first_pass(g_buf, zpg.at[1], b))

    reach = (lax.broadcasted_iota(jnp.int32, (LAGS, LAGS), 0) - LAGS // 2).astype(F32)
    unit = 1.0 / (512.0 * 512.0 * 512.0)

    def lag_table(r):
        return (lag_cos[...] * u_s[pl.ds(r, 1), :] + lag_sin[...] * v_s[pl.ds(r, 1), :]).astype(BF16)

    @pl.loop(0, 8)
    def _(n):
        t = n // 4
        i = (n // 2) % 2
        j = n % 2
        tile = x_lo + t * (1 - 2 * x_lo)
        at_m = al((tile * 2 + j) * 256)
        at_x = al(j * 256)
        a_s[...] = jnp.dot(zm[i, :, pl.ds(at_m, 512)], table_t[...], preferred_element_type=F32)
        b_s[...] = jnp.dot(zpg[t, i, :, pl.ds(at_x, 512)], table_t[...], preferred_element_type=F32)

        @pl.loop(0, 8)
        def _(rc):
            for kb in range(2):
                for lb in range(2):
                    cross_chunk(a_s, b_s, mix, kb, lb, rc)

        rows = lag_table(8 * t + i * 2 + j)
        columns = lag_table(8 * t + 4 + i * 2 + j)
        half = jnp.dot(rows, mix[...], preferred_element_type=F32).astype(BF16)
        surface = lax.dot_general(half, columns, (((1,), (1,)), ((), ())), preferred_element_type=F32) * unit
        weights = surface * surface
        sums[0, pl.ds(n, 1), :] = jnp.sum(weights, axis=0, keepdims=True)
        sums[1, pl.ds(n, 1), :] = jnp.sum(weights * reach, axis=0, keepdims=True)

    lane = lax.broadcasted_iota(jnp.int32, (8, 128), 1)
    along = (lane - LAGS // 2).astype(F32)
    by_pair = sums[0]
    total = 1.0 + jnp.sum(by_pair, axis=1, keepdims=True)
    shift_r = jnp.sum(sums[1], axis=1, keepdims=True) / total
    shift_c = jnp.sum(by_pair * along, axis=1, keepdims=True) / total

    lane1 = lax.broadcasted_iota(jnp.int32, (1, 128), 1)
    guest_s = 3 - 2 * (gz + x_lo - 2 * gz * x_lo)
    for i in range(2):
        line = jnp.zeros((1, 128), F32)
        for t in range(2):
            s = 2 * gz if t == 0 else guest_s
            c_tile = 2 * z + (x_lo if t == 0 else 1 - x_lo)
            held = prior_own[0] if t == 0 else prior_guest[...]
            for j in range(2):
                n = t * 4 + i * 2 + j
                r = i * 2 + j
                place = s * 16 + 2 * c_tile + j
                flow_r = held[r : r + 1, :].astype(F32) + shift_r[n : n + 1, :]
                flow_c = held[4 + r : 5 + r, :].astype(F32) + shift_c[n : n + 1, :]
                line = line + jnp.where(lane1 == place, flow_r, 0.0) + jnp.where(lane1 == place + 64, flow_c, 0.0)
        flow_send[i : i + 1, :] = line

    me_plane = gz * n_col + col

    def to_plane(d, peer):
        return pltpu.make_async_remote_copy(
            src_ref=flow_send, dst_ref=flow_recv.at[me_plane], send_sem=send_p.at[d], recv_sem=recv_p.at[d],
            device_id=peer, device_id_type=MESH,
        )

    offsets = [(dg, dc) for dg in range(n_gz) for dc in range(n_col) if dg or dc]
    for d, peer in enumerate(peers_plane):
        to_plane(d, peer).start()
    lines = flow_send[...]
    for d, (dg, dc) in enumerate(offsets):
        source = lax.rem(gz + n_gz - dg, n_gz) * n_col + lax.rem(col + n_col - dc, n_col)
        pltpu.make_async_remote_copy(
            src_ref=flow_recv.at[source], dst_ref=flow_recv.at[source], send_sem=send_p.at[d], recv_sem=recv_p.at[d],
            device_id=a_id, device_id_type=MESH,
        ).wait_recv()
        lines = lines + flow_recv[source]
    grid_send[...] = lines

    def to_column(d, peer):
        return pltpu.make_async_remote_copy(
            src_ref=grid_send, dst_ref=grid_recv.at[row], send_sem=send_c.at[d], recv_sem=recv_c.at[d],
            device_id=peer, device_id_type=MESH,
        )

    for d, peer in enumerate(peers_column):
        to_column(d, peer).start()
    want = [row_order[2 * row + m] for m in range(2)]
    picked = [jnp.zeros((1, 128), F32) for _ in range(2)]

    def pick(block, owner):
        for m in range(2):
            for i in range(2):
                hit = jnp.full((1, 128), want[m], jnp.int32) == jnp.full((1, 128), 2 * owner + i, jnp.int32)
                picked[m] = picked[m] + jnp.where(hit, block[i : i + 1, :], 0.0)

    pick(lines, row)
    for d in range(n_row - 1):
        source = lax.rem(row + n_row - (d + 1), n_row)
        pltpu.make_async_remote_copy(
            src_ref=grid_recv.at[source], dst_ref=grid_recv.at[source], send_sem=send_c.at[d], recv_sem=recv_c.at[d],
            device_id=a_id, device_id_type=MESH,
        ).wait_recv()
        pick(grid_recv[source], source)
    for m in range(2):
        out[m : m + 1, :] = picked[m]

    sends = [
        (pa_outer, None), (pa_near, None), (m_a, None), (m_n, has_out), (pa_mid, None), (mz_own, has_out), (mb_tile, None),
        (mz_guest, has_in), (mb_near, None), (mb_far, has_out), (prior_send, None),
    ]
    for copy, cond in sends:
        if cond is None:
            copy.wait_send()
        else:
            pl.when(cond)(copy.wait_send)
    for k in range(12):
        guarded(k, functools.partial(wait_sent_rows, k))
    for d, peer in enumerate(peers_plane):
        to_plane(d, peer).wait_send()
    for d, peer in enumerate(peers_column):
        to_column(d, peer).wait_send()


def body(sections, priors, row_order):
    table = forward_table()
    lag_cos, lag_sin = lag_tables()
    vmem = pl.BlockSpec(memory_space=pltpu.VMEM)
    smem = pl.BlockSpec(memory_space=pltpu.SMEM)
    dma = pltpu.SemaphoreType.DMA
    return pl.pallas_call(
        kernel,
        out_shape=jax.ShapeDtypeStruct((2, 128), F32),
        in_specs=[pl.BlockSpec(memory_space=pl.ANY), smem, smem, vmem, vmem, vmem, vmem, vmem],
        out_specs=vmem,
        scratch_shapes=[
            pltpu.VMEM((768, 1280), BF16),
            pltpu.VMEM((2, 768, 768), BF16),
            pltpu.VMEM((2, 512, 1280), BF16),
            pltpu.VMEM((2, 2, 512, 768), BF16),
            pltpu.VMEM((512, 512), F32),
            pltpu.VMEM((512, 512), F32),
            pltpu.VMEM((512, 512), BF16),
            pltpu.VMEM((2, 8, 128), jnp.int32),
            pltpu.VMEM((8, 128), jnp.int32),
            pltpu.VMEM((16, 512), F32),
            pltpu.VMEM((16, 512), F32),
            pltpu.VMEM((2, 8, 128), F32),
            pltpu.VMEM((2, 128), F32),
            pltpu.VMEM((16, 2, 128), F32),
            pltpu.VMEM((2, 128), F32),
            pltpu.VMEM((8, 2, 128), F32),
            dma((2,)),
            dma((11,)),
            dma((11,)),
            dma((24,)),
            dma((24,)),
            dma((15,)),
            dma((15,)),
            dma((7,)),
            dma((7,)),
        ],
        compiler_params=pltpu.CompilerParams(collective_id=0, has_side_effects=True, vmem_limit_bytes=48 * 1024 * 1024),
    )(
        sections, priors, row_order, jnp.asarray(table), jnp.asarray(np.ascontiguousarray(table.T)),
        jnp.asarray(lag_cos), jnp.asarray(lag_sin), jnp.asarray(phase_rows()),
    )


def solution(mesh):
    return jax.shard_map(
        body,
        mesh=mesh,
        in_specs=(P("gz", "row", "col"), P(None, "gz", "row", "col"), P()),
        out_specs=P("row", None),
        check_vma=False,
    )
```

```python
import functools

import jax
import jax.numpy as jnp
import ml_dtypes
import numpy as np
from jax import lax
from jax.experimental import pallas as pl
from jax.experimental.pallas import tpu as pltpu
from jax.sharding import PartitionSpec as P

PATCH = 512
LAGS = 128
UNIT = 128
MESH = pl.DeviceIdType.MESH
BF16 = jnp.bfloat16
F32 = jnp.float32


def slots():
    m = np.arange(128)
    freq = np.concatenate([2 * m, 2 * m, 2 * m + 1, 2 * m + 1])
    sine = np.concatenate([np.zeros(128), np.ones(128), np.zeros(128), np.ones(128)]).astype(bool)
    weight = np.full(512, 2.0)
    freq[128], sine[128] = 256, False
    weight[0] = weight[128] = 1.0
    return freq, sine, weight


def forward_table():
    freq, sine, _ = slots()
    angle = (freq[:, None] * np.arange(PATCH)[None, :]) % PATCH * (2.0 * np.pi / PATCH)
    return np.where(sine[:, None], np.sin(angle), np.cos(angle)).astype(ml_dtypes.bfloat16)


def lag_tables():
    freq, _, weight = slots()
    lag = np.arange(LAGS) - LAGS // 2
    angle = (freq[None, :] * lag[:, None]) % PATCH * (2.0 * np.pi / PATCH)
    return (np.cos(angle) * weight).astype(np.float32), (np.sin(angle) * weight).astype(np.float32)


def phase_rows():
    freq, sine, _ = slots()
    rows = np.zeros((8, 512), np.int32)
    rows[0] = freq
    rows[1] = np.where(sine, -128, 0)
    rows[2] = np.where(sine, 0, 128)
    rows[3] = 1
    rows[3, 128] = 0
    return rows


def cross_chunk(a, b, m_ref, kb, lb, rc):
    lc, ls = pl.ds(lb * 256, 128), pl.ds(lb * 256 + 128, 128)
    rt, rl = pl.ds(rc * 16, 16), pl.ds(128 + rc * 16, 16)
    mt, ml = pl.ds(kb * 256 + rc * 16, 16), pl.ds(kb * 256 + 128 + rc * 16, 16)
    a1, a2, a3, a4 = a[rt, lc], a[rt, ls], a[rl, lc], a[rl, ls]
    b1, b2, b3, b4 = b[rt, lc], b[rt, ls], b[rl, lc], b[rl, ls]
    p33, p44 = a3 * b3, a4 * b4
    u1, u2 = a1 * b2 - a2 * b1, a3 * b4 - a4 * b3
    v1, v2 = a1 * b3 - a3 * b1, a2 * b4 - a4 * b2
    ss = (a1 * b4 + a4 * b1) - (a2 * b3 + a3 * b2)
    first_row = kb == 0 and rc == 0
    if first_row:
        k0 = lax.broadcasted_iota(jnp.int32, (16, 128), 0) == 0
        z33, z44, zu2 = jnp.where(k0, 0.0, p33), jnp.where(k0, 0.0, p44), jnp.where(k0, 0.0, u2)
    else:
        z33, z44, zu2 = p33, p44, u2
    t1, t2 = a1 * b1 + z33, a2 * b2 + z44
    cc, cs, sc = t1 + t2, u1 + zu2, v1 + v2
    if first_row:
        sc, ss = jnp.where(k0, p33 + p44, sc), jnp.where(k0, u2, ss)
    if lb == 0:
        l0 = lax.broadcasted_iota(jnp.int32, (16, 128), 1) == 0
        cc, cs = jnp.where(l0, t1, cc), jnp.where(l0, t2, cs)
        if first_row:
            sc = jnp.where(l0, jnp.where(k0, p33, v1), sc)
            ss = jnp.where(l0, jnp.where(k0, p44, v2), ss)
        else:
            sc, ss = jnp.where(l0, v1, sc), jnp.where(l0, v2, ss)
    m_ref[mt, lc] = cc.astype(BF16)
    m_ref[mt, ls] = cs.astype(BF16)
    m_ref[ml, lc] = sc.astype(BF16)
    m_ref[ml, ls] = ss.astype(BF16)


def kernel(
    sections, priors_h, row_order_h, table_h, table_t_h, lag_cos_h, lag_sin_h, phases_h, out,
    priors, row_order, table, table_t, lag_cos, lag_sin, phases, m_buf, pg_buf, zm, zpg, a_s, b_s, mix, prior_own, prior_guest, u_s, v_s, sums, flow_send, flow_recv, grid_send, grid_recv,
    local_sem, send_x, recv_x, send_r, recv_r, send_p, recv_p, send_c, recv_c,
):
    gz, row, col = lax.axis_index("gz"), lax.axis_index("row"), lax.axis_index("col")
    n_gz, n_row, n_col = lax.axis_size("gz"), lax.axis_size("row"), lax.axis_size("col")
    x_lo = lax.rem(col, 2)
    z = lax.div(col, 2)
    has_left, has_right = z > 0, z < n_col // 2 - 1
    has_out = jnp.logical_or(jnp.logical_and(x_lo == 0, has_left), jnp.logical_and(x_lo == 1, has_right))
    has_in = jnp.logical_or(jnp.logical_and(x_lo == 1, has_left), jnp.logical_and(x_lo == 0, has_right))
    has_up, has_down = row > 0, row < n_row - 1
    side = 2 * x_lo - 1
    a_id = (gz, row, col - side)
    b_id = (1 - gz, row, col - side)
    n_id = (gz, row, col + side)
    z_out = (gz, row, col + 2 * side)
    z_in = (gz, row, col - 2 * side)
    up_id, down_id = (gz, row - 1, col), (gz, row + 1, col)

    def al(v):
        return pl.multiple_of(v, 128)

    c0 = al(128 + 512 * x_lo)
    near, outer = al(512 + 128 * x_lo), al(128 + 896 * x_lo)
    near_p, outer_p = al(512 - 384 * x_lo), al(128 + 384 * x_lo)
    c1 = al(640 - 512 * x_lo)
    near_g, outer_g = al(640 - 128 * x_lo), al(1024 - 896 * x_lo)
    m_far_out, m_far_in = al(1152 * x_lo), al(1152 - 1152 * x_lo)
    side_in, side_out = al(640 - 640 * x_lo), al(640 * x_lo)
    body = pl.ds(128, 512)
    p_buf, g_buf = pg_buf.at[0], pg_buf.at[1]

    own_m = pltpu.make_async_copy(sections.at[x_lo], m_buf.at[body, pl.ds(c0, 512)], local_sem.at[0])
    own_p = pltpu.make_async_copy(sections.at[1 - x_lo], p_buf.at[body, pl.ds(128, 512)], local_sem.at[1])
    own_m.start()
    own_p.start()
    constants = [
        pltpu.make_async_copy(src, dst, local_sem.at[2 + k])
        for k, (src, dst) in enumerate([
            (priors_h, priors), (phases_h, phases), (table_h, table), (table_t_h, table_t),
            (lag_cos_h, lag_cos), (lag_sin_h, lag_sin), (row_order_h, row_order),
        ])
    ]
    for copy in constants:
        copy.start()

    peers_plane = [(lax.rem(gz + dg, n_gz), row, lax.rem(col + dc, n_col)) for dg in range(n_gz) for dc in range(n_col) if dg or dc]
    peers_column = [(gz, lax.rem(row + d, n_row), col) for d in range(1, n_row)]
    barrier = pltpu.get_barrier_semaphore()
    for peer in peers_plane + peers_column:
        pl.semaphore_signal(barrier, inc=1, device_id=peer, device_id_type=MESH)

    constants[0].wait()
    for c in range(2):
        for ii in range(2):
            for jj in range(2):
                r = c * 4 + ii * 2 + jj
                prior_own[0, r : r + 1, :] = jnp.full((1, 128), priors[c, 0, ii, jj], jnp.int32)
                prior_own[1, r : r + 1, :] = jnp.full((1, 128), priors[c, 1, ii, jj], jnp.int32)

    @pl.when(row == 0)
    def _():
        m_buf[0:128, :] = jnp.zeros((128, 1280), BF16)
        pg_buf[:, 0:128, :] = jnp.zeros((2, 128, 768), BF16)

    @pl.when(row == n_row - 1)
    def _():
        m_buf[640:768, :] = jnp.zeros((128, 1280), BF16)
        pg_buf[:, 640:768, :] = jnp.zeros((2, 128, 768), BF16)

    @pl.when(jnp.logical_not(has_left))
    def _():
        m_buf[:, 0:128] = jnp.zeros((768, 128), BF16)
        pg_buf[x_lo, :, 0:128] = jnp.zeros((768, 128), BF16)

    @pl.when(jnp.logical_not(has_right))
    def _():
        m_buf[:, 1152:1280] = jnp.zeros((768, 128), BF16)
        pg_buf[1 - x_lo, :, 640:768] = jnp.zeros((768, 128), BF16)

    own_m.wait()
    own_p.wait()
    pl.semaphore_wait(barrier, len(peers_plane) + len(peers_column))

    def remote(k, src, dst, device):
        return pltpu.make_async_remote_copy(
            src_ref=src, dst_ref=dst, send_sem=send_x.at[k], recv_sem=recv_x.at[k], device_id=device, device_id_type=MESH
        )

    def strip(ref, start, width=128):
        return ref.at[body, pl.ds(start, width)]

    pa_outer = remote(0, strip(p_buf, outer_p), strip(m_buf, outer), a_id)
    pa_near = remote(1, strip(p_buf, near_p), strip(m_buf, near), a_id)
    m_a = remote(2, strip(m_buf, near), strip(p_buf, side_out), a_id)
    m_n = remote(3, strip(m_buf, outer), strip(p_buf, side_in), n_id)
    pa_mid = remote(4, strip(p_buf, 256, 256), strip(m_buf, al(c0 + 128), 256), a_id)
    mz_own = remote(5, strip(m_buf, outer), strip(m_buf, m_far_in), z_out)
    mb_tile = remote(6, strip(m_buf, c0, 512), strip(g_buf, 128, 512), b_id)
    mz_guest = remote(7, strip(m_buf, outer_g), strip(m_buf, m_far_out), z_in)
    mb_near = remote(8, strip(m_buf, near_g), strip(g_buf, side_in), b_id)
    mb_far = remote(9, strip(m_buf, m_far_out), strip(g_buf, side_out), b_id)
    prior_id = (gz + x_lo * (1 - 2 * gz), row, col - side)
    prior_send = remote(10, prior_own.at[1], prior_guest, prior_id)

    prior_send.start()
    pa_outer.start()
    mb_tile.start()
    pl.when(has_out)(mz_own.start)
    pa_near.start()
    m_a.start()
    pl.when(has_out)(m_n.start)
    pa_mid.start()

    landed = {
        0: strip(m_buf, outer_g), 1: strip(m_buf, near_g), 2: strip(p_buf, side_in), 3: strip(p_buf, side_out),
        4: strip(m_buf, al(c1 + 128), 256), 5: strip(m_buf, m_far_in), 6: strip(g_buf, 128, 512), 7: strip(m_buf, m_far_out),
        8: strip(g_buf, side_out), 9: strip(g_buf, side_in), 10: prior_guest,
    }
    when_recv = {3: has_out, 5: has_in, 7: has_out, 9: has_in}

    def landing(k):
        ref = landed[k]
        return remote(k, ref, ref, a_id)

    def rows_of(k, ref, start, width):
        cols = pl.ds(start, width)
        up = pltpu.make_async_remote_copy(
            src_ref=ref.at[pl.ds(128, 128), cols], dst_ref=ref.at[pl.ds(640, 128), cols],
            send_sem=send_r.at[2 * k], recv_sem=recv_r.at[2 * k], device_id=up_id, device_id_type=MESH,
        )
        down = pltpu.make_async_remote_copy(
            src_ref=ref.at[pl.ds(512, 128), cols], dst_ref=ref.at[pl.ds(0, 128), cols],
            send_sem=send_r.at[2 * k + 1], recv_sem=recv_r.at[2 * k + 1], device_id=down_id, device_id_type=MESH,
        )
        return up, down

    pieces = {
        0: (m_buf, outer_g, 128), 1: (m_buf, near_g, 128), 2: (p_buf, side_in, 128), 3: (p_buf, side_out, 128),
        4: (m_buf, al(c1 + 128), 256), 5: (m_buf, m_far_in, 128), 6: (g_buf, 128, 512), 7: (m_buf, m_far_out, 128),
        8: (g_buf, side_out, 128), 9: (g_buf, side_in, 128), 10: (m_buf, c0, 512), 11: (p_buf, 128, 512),
    }

    def send_rows(k):
        up, down = rows_of(k, *pieces[k])
        pl.when(has_up)(up.start)
        pl.when(has_down)(down.start)

    def wait_rows(k):
        up, down = rows_of(k, *pieces[k])
        pl.when(has_down)(up.wait_recv)
        pl.when(has_up)(down.wait_recv)

    def wait_sent_rows(k):
        up, down = rows_of(k, *pieces[k])
        pl.when(has_up)(up.wait_send)
        pl.when(has_down)(down.wait_send)

    def guarded(k, do):
        if k in when_recv:
            pl.when(when_recv[k])(do)
        else:
            do()

    def arrive(k, forward=None, cond=None):
        def do():
            landing(k).wait_recv()
            send_rows(k)

        guarded(k, do)
        if forward is not None:
            if cond is None:
                forward.start()
            else:
                pl.when(cond)(forward.start)

    send_rows(10)
    send_rows(11)
    landing(10).wait_recv()

    for copy in constants[1:]:
        copy.wait()
    freq, off_u, off_v, mask_v = phases[0:1, :], phases[1:2, :], phases[2:3, :], phases[3:4, :]
    for t in range(2):
        value = prior_own[0] if t == 0 else prior_guest[...]
        sign = (1 - 2 * x_lo) * (1 - 2 * t)
        wide = jnp.concatenate([value] * 4, axis=1) * sign
        turn = wide * freq
        scale = 2.0 * np.pi / PATCH
        u_s[8 * t : 8 * t + 8, :] = jnp.cos(((turn + off_u) & (PATCH - 1)).astype(F32) * scale)
        v_s[8 * t : 8 * t + 8, :] = (
            jnp.cos(((turn + off_v) & (PATCH - 1)).astype(F32) * scale) * mask_v.astype(F32) * sign.astype(F32)
        )

    reach = (lax.broadcasted_iota(jnp.int32, (LAGS, LAGS), 0) - LAGS // 2).astype(F32)
    unit = 1.0 / (512.0 * 512.0 * 512.0)

    def first_pass(src, dst, block):
        at = al(block * 256)
        for i in range(2):
            dst[i, :, pl.ds(at, 256)] = jnp.dot(
                table[...], src[pl.ds(256 * i, 512), pl.ds(at, 256)], preferred_element_type=F32
            ).astype(BF16)

    def rows_in(*ks):
        for k in ks:
            guarded(k, functools.partial(wait_rows, k))

    def lag_table(r):
        return (lag_cos[...] * u_s[pl.ds(r, 1), :] + lag_sin[...] * v_s[pl.ds(r, 1), :]).astype(BF16)

    def pairs(t, j, between=None):
        tile = x_lo if t == 0 else 1 - x_lo
        at_m, at_x = al((tile * 2 + j) * 256), al(j * 256)

        def spectra(h):
            i, kb = h // 2, h % 2
            rows = pl.ds(kb * 256, 256)
            a_s[h % 2] = jnp.dot(zm[i, rows, pl.ds(at_m, 512)], table_t[...], preferred_element_type=F32)
            b_s[h % 2] = jnp.dot(zpg[t, i, rows, pl.ds(at_x, 512)], table_t[...], preferred_element_type=F32)

        def products(h):
            for rc in range(8):
                for lb in range(2):
                    cross_chunk(a_s.at[h % 2], b_s.at[h % 2], mix.at[h // 2], h % 2, lb, rc)

        def window(i):
            n = t * 4 + i * 2 + j
            rows = lag_table(8 * t + i * 2 + j)
            columns = lag_table(8 * t + 4 + i * 2 + j)
            half = jnp.dot(rows, mix[i], preferred_element_type=F32).astype(BF16)
            surface = lax.dot_general(half, columns, (((1,), (1,)), ((), ())), preferred_element_type=F32) * unit
            weights = surface * surface
            sums[0, pl.ds(n, 1), :] = jnp.sum(weights, axis=0, keepdims=True)
            sums[1, pl.ds(n, 1), :] = jnp.sum(weights * reach, axis=0, keepdims=True)

        spectra(0)
        spectra(1)
        products(0)
        spectra(2)
        products(1)
        if between is not None:
            between()
        spectra(3)
        window(0)
        products(2)
        products(3)
        window(1)

    rows_in(10, 11)
    first_pass(m_buf, zm, 1 + 2 * x_lo)
    first_pass(p_buf, zpg.at[0], 1)
    arrive(0, mz_guest, has_in)
    arrive(5)
    arrive(1, mb_near)
    rows_in(0, 5)
    first_pass(m_buf, zm, 4 - 4 * x_lo)
    arrive(7, mb_far, has_out)
    rows_in(1)
    first_pass(m_buf, zm, 2)
    arrive(2)
    rows_in(7)
    first_pass(m_buf, zm, 4 * x_lo)
    rows_in(2)
    first_pass(p_buf, zpg.at[0], 2 - 2 * x_lo)

    def arrivals():
        arrive(3)
        arrive(6)

    pairs(0, 1 - x_lo, arrivals)
    rows_in(3)
    first_pass(p_buf, zpg.at[0], 2 * x_lo)
    rows_in(6)
    first_pass(g_buf, zpg.at[1], 1)
    pairs(0, x_lo)
    arrive(4)
    arrive(8)
    arrive(9)
    rows_in(4)
    first_pass(m_buf, zm, 3 - 2 * x_lo)
    rows_in(8)
    first_pass(g_buf, zpg.at[1], 2 * x_lo)
    pairs(1, x_lo)
    rows_in(9)
    first_pass(g_buf, zpg.at[1], 2 - 2 * x_lo)
    pairs(1, 1 - x_lo)

    lane = lax.broadcasted_iota(jnp.int32, (8, 128), 1)
    along = (lane - LAGS // 2).astype(F32)
    by_pair = sums[0]
    total = 1.0 + jnp.sum(by_pair, axis=1, keepdims=True)
    shift_r = jnp.sum(sums[1], axis=1, keepdims=True) / total
    shift_c = jnp.sum(by_pair * along, axis=1, keepdims=True) / total

    lane1 = lax.broadcasted_iota(jnp.int32, (1, 128), 1)
    guest_s = 3 - 2 * (gz + x_lo - 2 * gz * x_lo)
    for i in range(2):
        line = jnp.zeros((1, 128), F32)
        for t in range(2):
            s = 2 * gz if t == 0 else guest_s
            c_tile = 2 * z + (x_lo if t == 0 else 1 - x_lo)
            held = prior_own[0] if t == 0 else prior_guest[...]
            for j in range(2):
                n = t * 4 + i * 2 + j
                r = i * 2 + j
                place = s * 16 + 2 * c_tile + j
                flow_r = held[r : r + 1, :].astype(F32) + shift_r[n : n + 1, :]
                flow_c = held[4 + r : 5 + r, :].astype(F32) + shift_c[n : n + 1, :]
                line = line + jnp.where(lane1 == place, flow_r, 0.0) + jnp.where(lane1 == place + 64, flow_c, 0.0)
        flow_send[i : i + 1, :] = line

    me_plane = gz * n_col + col

    def to_plane(d, peer):
        return pltpu.make_async_remote_copy(
            src_ref=flow_send, dst_ref=flow_recv.at[me_plane], send_sem=send_p.at[d], recv_sem=recv_p.at[d],
            device_id=peer, device_id_type=MESH,
        )

    offsets = [(dg, dc) for dg in range(n_gz) for dc in range(n_col) if dg or dc]
    for d, peer in enumerate(peers_plane):
        to_plane(d, peer).start()
    lines = flow_send[...]
    for d, (dg, dc) in enumerate(offsets):
        source = lax.rem(gz + n_gz - dg, n_gz) * n_col + lax.rem(col + n_col - dc, n_col)
        pltpu.make_async_remote_copy(
            src_ref=flow_recv.at[source], dst_ref=flow_recv.at[source], send_sem=send_p.at[d], recv_sem=recv_p.at[d],
            device_id=a_id, device_id_type=MESH,
        ).wait_recv()
        lines = lines + flow_recv[source]
    grid_send[...] = lines

    def to_column(d, peer):
        return pltpu.make_async_remote_copy(
            src_ref=grid_send, dst_ref=grid_recv.at[row], send_sem=send_c.at[d], recv_sem=recv_c.at[d],
            device_id=peer, device_id_type=MESH,
        )

    for d, peer in enumerate(peers_column):
        to_column(d, peer).start()
    want = [row_order[2 * row + m] for m in range(2)]
    picked = [jnp.zeros((1, 128), F32) for _ in range(2)]

    def pick(block, owner):
        for m in range(2):
            for i in range(2):
                hit = jnp.full((1, 128), want[m], jnp.int32) == jnp.full((1, 128), 2 * owner + i, jnp.int32)
                picked[m] = picked[m] + jnp.where(hit, block[i : i + 1, :], 0.0)

    pick(lines, row)
    for d in range(n_row - 1):
        source = lax.rem(row + n_row - (d + 1), n_row)
        pltpu.make_async_remote_copy(
            src_ref=grid_recv.at[source], dst_ref=grid_recv.at[source], send_sem=send_c.at[d], recv_sem=recv_c.at[d],
            device_id=a_id, device_id_type=MESH,
        ).wait_recv()
        pick(grid_recv[source], source)
    for m in range(2):
        out[m : m + 1, :] = picked[m]

    sends = [
        (pa_outer, None), (pa_near, None), (m_a, None), (m_n, has_out), (pa_mid, None), (mz_own, has_out), (mb_tile, None),
        (mz_guest, has_in), (mb_near, None), (mb_far, has_out), (prior_send, None),
    ]
    for copy, cond in sends:
        if cond is None:
            copy.wait_send()
        else:
            pl.when(cond)(copy.wait_send)
    for k in range(12):
        guarded(k, functools.partial(wait_sent_rows, k))
    for d, peer in enumerate(peers_plane):
        to_plane(d, peer).wait_send()
    for d, peer in enumerate(peers_column):
        to_column(d, peer).wait_send()


def body(sections, priors, row_order):
    table = forward_table()
    lag_cos, lag_sin = lag_tables()
    vmem = pl.BlockSpec(memory_space=pltpu.VMEM)
    dma = pltpu.SemaphoreType.DMA
    return pl.pallas_call(
        kernel,
        out_shape=jax.ShapeDtypeStruct((2, 128), F32),
        in_specs=[pl.BlockSpec(memory_space=pltpu.HBM)] * 8,
        out_specs=vmem,
        scratch_shapes=[
            pltpu.SMEM((2, 2, 2, 2), jnp.int32),
            pltpu.SMEM((16,), jnp.int32),
            pltpu.VMEM((512, 512), BF16),
            pltpu.VMEM((512, 512), BF16),
            pltpu.VMEM((LAGS, 512), F32),
            pltpu.VMEM((LAGS, 512), F32),
            pltpu.VMEM((8, 512), jnp.int32),
            pltpu.VMEM((768, 1280), BF16),
            pltpu.VMEM((2, 768, 768), BF16),
            pltpu.VMEM((2, 512, 1280), BF16),
            pltpu.VMEM((2, 2, 512, 768), BF16),
            pltpu.VMEM((2, 256, 512), F32),
            pltpu.VMEM((2, 256, 512), F32),
            pltpu.VMEM((2, 512, 512), BF16),
            pltpu.VMEM((2, 8, 128), jnp.int32),
            pltpu.VMEM((8, 128), jnp.int32),
            pltpu.VMEM((16, 512), F32),
            pltpu.VMEM((16, 512), F32),
            pltpu.VMEM((2, 8, 128), F32),
            pltpu.VMEM((2, 128), F32),
            pltpu.VMEM((16, 2, 128), F32),
            pltpu.VMEM((2, 128), F32),
            pltpu.VMEM((8, 2, 128), F32),
            dma((9,)),
            dma((11,)),
            dma((11,)),
            dma((24,)),
            dma((24,)),
            dma((15,)),
            dma((15,)),
            dma((7,)),
            dma((7,)),
        ],
        compiler_params=pltpu.CompilerParams(collective_id=0, has_side_effects=True, vmem_limit_bytes=67_043_328),
    )(
        sections, priors, row_order, jnp.asarray(table), jnp.asarray(np.ascontiguousarray(table.T)),
        jnp.asarray(lag_cos), jnp.asarray(lag_sin), jnp.asarray(phase_rows()),
    )


def solution(mesh):
    return jax.shard_map(
        body,
        mesh=mesh,
        in_specs=(P("gz", "row", "col"), P(None, "gz", "row", "col"), P()),
        out_specs=P("row", None),
        check_vma=False,
    )
```

```python
import functools

import jax
import jax.numpy as jnp
import ml_dtypes
import numpy as np
from jax import lax
from jax.experimental import pallas as pl
from jax.experimental.pallas import tpu as pltpu
from jax.sharding import PartitionSpec as P

PATCH = 512
LAGS = 128
UNIT = 128
MESH = pl.DeviceIdType.MESH
BF16 = jnp.bfloat16
F32 = jnp.float32


def slots():
    m = np.arange(128)
    freq = np.concatenate([2 * m, 2 * m, 2 * m + 1, 2 * m + 1])
    sine = np.concatenate([np.zeros(128), np.ones(128), np.zeros(128), np.ones(128)]).astype(bool)
    weight = np.full(512, 2.0)
    freq[128], sine[128] = 256, False
    weight[0] = weight[128] = 1.0
    return freq, sine, weight


def forward_table():
    freq, sine, _ = slots()
    angle = (freq[:, None] * np.arange(PATCH)[None, :]) % PATCH * (2.0 * np.pi / PATCH)
    return np.where(sine[:, None], np.sin(angle), np.cos(angle)).astype(ml_dtypes.bfloat16)


def lag_tables():
    freq, _, weight = slots()
    lag = np.arange(LAGS) - LAGS // 2
    angle = (freq[None, :] * lag[:, None]) % PATCH * (2.0 * np.pi / PATCH)
    return (np.cos(angle) * weight).astype(np.float32), (np.sin(angle) * weight).astype(np.float32)


def phase_rows():
    freq, sine, _ = slots()
    rows = np.zeros((8, 512), np.int32)
    rows[0] = freq
    rows[1] = np.where(sine, -128, 0)
    rows[2] = np.where(sine, 0, 128)
    rows[3] = 1
    rows[3, 128] = 0
    return rows


def cross_chunk(a, b, m_ref, kb, lb, rc):
    lc, ls = pl.ds(lb * 256, 128), pl.ds(lb * 256 + 128, 128)
    rt, rl = pl.ds(rc * 16, 16), pl.ds(128 + rc * 16, 16)
    mt, ml = pl.ds(kb * 256 + rc * 16, 16), pl.ds(kb * 256 + 128 + rc * 16, 16)
    a1, a2, a3, a4 = a[rt, lc], a[rt, ls], a[rl, lc], a[rl, ls]
    b1, b2, b3, b4 = b[rt, lc], b[rt, ls], b[rl, lc], b[rl, ls]
    p33, p44 = a3 * b3, a4 * b4
    u1, u2 = a1 * b2 - a2 * b1, a3 * b4 - a4 * b3
    v1, v2 = a1 * b3 - a3 * b1, a2 * b4 - a4 * b2
    ss = (a1 * b4 + a4 * b1) - (a2 * b3 + a3 * b2)
    first_row = kb == 0 and rc == 0
    if first_row:
        k0 = lax.broadcasted_iota(jnp.int32, (16, 128), 0) == 0
        z33, z44, zu2 = jnp.where(k0, 0.0, p33), jnp.where(k0, 0.0, p44), jnp.where(k0, 0.0, u2)
    else:
        z33, z44, zu2 = p33, p44, u2
    t1, t2 = a1 * b1 + z33, a2 * b2 + z44
    cc, cs, sc = t1 + t2, u1 + zu2, v1 + v2
    if first_row:
        sc, ss = jnp.where(k0, p33 + p44, sc), jnp.where(k0, u2, ss)
    if lb == 0:
        l0 = lax.broadcasted_iota(jnp.int32, (16, 128), 1) == 0
        cc, cs = jnp.where(l0, t1, cc), jnp.where(l0, t2, cs)
        if first_row:
            sc = jnp.where(l0, jnp.where(k0, p33, v1), sc)
            ss = jnp.where(l0, jnp.where(k0, p44, v2), ss)
        else:
            sc, ss = jnp.where(l0, v1, sc), jnp.where(l0, v2, ss)
    m_ref[mt, lc] = cc.astype(BF16)
    m_ref[mt, ls] = cs.astype(BF16)
    m_ref[ml, lc] = sc.astype(BF16)
    m_ref[ml, ls] = ss.astype(BF16)


def kernel(
    sections, priors_h, row_order_h, table_h, table_t_h, lag_cos_h, lag_sin_h, phases_h, out,
    priors, row_order, table, table_t, lag_cos, lag_sin, phases, m_buf, pg_buf, zm, zpg, a_s, b_s, mix, prior_own, prior_guest, u_s, v_s, sums, flow_send, flow_recv, known,
    local_sem, send_x, recv_x, send_r, recv_r, send_f, recv_f,
):
    gz, row, col = lax.axis_index("gz"), lax.axis_index("row"), lax.axis_index("col")
    n_gz, n_row, n_col = lax.axis_size("gz"), lax.axis_size("row"), lax.axis_size("col")
    x_lo = lax.rem(col, 2)
    z = lax.div(col, 2)
    has_left, has_right = z > 0, z < n_col // 2 - 1
    has_out = jnp.logical_or(jnp.logical_and(x_lo == 0, has_left), jnp.logical_and(x_lo == 1, has_right))
    has_in = jnp.logical_or(jnp.logical_and(x_lo == 1, has_left), jnp.logical_and(x_lo == 0, has_right))
    has_up, has_down = row > 0, row < n_row - 1
    side = 2 * x_lo - 1
    a_id = (gz, row, col - side)
    b_id = (1 - gz, row, col - side)
    n_id = (gz, row, col + side)
    z_out = (gz, row, col + 2 * side)
    z_in = (gz, row, col - 2 * side)
    up_id, down_id = (gz, row - 1, col), (gz, row + 1, col)

    def al(v):
        return pl.multiple_of(v, 128)

    c0 = al(128 + 512 * x_lo)
    near, outer = al(512 + 128 * x_lo), al(128 + 896 * x_lo)
    near_p, outer_p = al(512 - 384 * x_lo), al(128 + 384 * x_lo)
    c1 = al(640 - 512 * x_lo)
    near_g, outer_g = al(640 - 128 * x_lo), al(1024 - 896 * x_lo)
    m_far_out, m_far_in = al(1152 * x_lo), al(1152 - 1152 * x_lo)
    side_in, side_out = al(640 - 640 * x_lo), al(640 * x_lo)
    body = pl.ds(128, 512)
    p_buf, g_buf = pg_buf.at[0], pg_buf.at[1]

    own_m = pltpu.make_async_copy(sections.at[x_lo], m_buf.at[body, pl.ds(c0, 512)], local_sem.at[0])
    own_p = pltpu.make_async_copy(sections.at[1 - x_lo], p_buf.at[body, pl.ds(128, 512)], local_sem.at[1])
    own_m.start()
    own_p.start()
    constants = [
        pltpu.make_async_copy(src, dst, local_sem.at[2 + k])
        for k, (src, dst) in enumerate([
            (priors_h, priors), (phases_h, phases), (table_h, table), (table_t_h, table_t),
            (lag_cos_h, lag_cos), (lag_sin_h, lag_sin), (row_order_h, row_order),
        ])
    ]
    for copy in constants:
        copy.start()

    def at(dg, dr, dc):
        return (lax.rem(gz + dg, n_gz), lax.rem(row + dr, n_row), lax.rem(col + dc, n_col))

    z_ring = [at(0, 0, 2), at(0, 0, n_col - 2)]
    row_ring = [at(0, 1, 0), at(0, n_row - 1, 0)]
    near_peers = [a_id, b_id, (gz, row, lax.rem(col + side + n_col, n_col))] + z_ring + row_ring
    barrier = pltpu.get_barrier_semaphore()
    for peer in near_peers:
        pl.semaphore_signal(barrier, inc=1, device_id=peer, device_id_type=MESH)

    rounds = [
        near_peers,
        [a_id, b_id, (1 - gz, row, col)],
        z_ring + [at(0, 0, n_col // 2)],
        [at(0, 2, 0), at(0, n_row - 2, 0)],
    ]

    def tell(k):
        for peer in rounds[k]:
            pl.semaphore_signal(known.at[k], inc=1, device_id=peer, device_id_type=MESH)

    def hear(k):
        pl.semaphore_wait(known.at[k], len(rounds[k]))

    constants[0].wait()
    for c in range(2):
        for ii in range(2):
            for jj in range(2):
                r = c * 4 + ii * 2 + jj
                prior_own[0, r : r + 1, :] = jnp.full((1, 128), priors[c, 0, ii, jj], jnp.int32)
                prior_own[1, r : r + 1, :] = jnp.full((1, 128), priors[c, 1, ii, jj], jnp.int32)

    @pl.when(row == 0)
    def _():
        m_buf[0:128, :] = jnp.zeros((128, 1280), BF16)
        pg_buf[:, 0:128, :] = jnp.zeros((2, 128, 768), BF16)

    @pl.when(row == n_row - 1)
    def _():
        m_buf[640:768, :] = jnp.zeros((128, 1280), BF16)
        pg_buf[:, 640:768, :] = jnp.zeros((2, 128, 768), BF16)

    @pl.when(jnp.logical_not(has_left))
    def _():
        m_buf[:, 0:128] = jnp.zeros((768, 128), BF16)
        pg_buf[x_lo, :, 0:128] = jnp.zeros((768, 128), BF16)

    @pl.when(jnp.logical_not(has_right))
    def _():
        m_buf[:, 1152:1280] = jnp.zeros((768, 128), BF16)
        pg_buf[1 - x_lo, :, 640:768] = jnp.zeros((768, 128), BF16)

    own_m.wait()
    own_p.wait()
    pl.semaphore_wait(barrier, len(near_peers))
    tell(0)

    def remote(k, src, dst, device):
        return pltpu.make_async_remote_copy(
            src_ref=src, dst_ref=dst, send_sem=send_x.at[k], recv_sem=recv_x.at[k], device_id=device, device_id_type=MESH
        )

    def strip(ref, start, width=128):
        return ref.at[body, pl.ds(start, width)]

    pa_outer = remote(0, strip(p_buf, outer_p), strip(m_buf, outer), a_id)
    pa_near = remote(1, strip(p_buf, near_p), strip(m_buf, near), a_id)
    m_a = remote(2, strip(m_buf, near), strip(p_buf, side_out), a_id)
    m_n = remote(3, strip(m_buf, outer), strip(p_buf, side_in), n_id)
    pa_mid = remote(4, strip(p_buf, 256, 256), strip(m_buf, al(c0 + 128), 256), a_id)
    mz_own = remote(5, strip(m_buf, outer), strip(m_buf, m_far_in), z_out)
    mb_tile = remote(6, strip(m_buf, c0, 512), strip(g_buf, 128, 512), b_id)
    mz_guest = remote(7, strip(m_buf, outer_g), strip(m_buf, m_far_out), z_in)
    mb_near = remote(8, strip(m_buf, near_g), strip(g_buf, side_in), b_id)
    mb_far = remote(9, strip(m_buf, m_far_out), strip(g_buf, side_out), b_id)
    prior_id = (gz + x_lo * (1 - 2 * gz), row, col - side)
    prior_send = remote(10, prior_own.at[1], prior_guest, prior_id)

    prior_send.start()
    pa_outer.start()
    mb_tile.start()
    pl.when(has_out)(mz_own.start)
    pa_near.start()
    m_a.start()
    pl.when(has_out)(m_n.start)
    pa_mid.start()

    landed = {
        0: strip(m_buf, outer_g), 1: strip(m_buf, near_g), 2: strip(p_buf, side_in), 3: strip(p_buf, side_out),
        4: strip(m_buf, al(c1 + 128), 256), 5: strip(m_buf, m_far_in), 6: strip(g_buf, 128, 512), 7: strip(m_buf, m_far_out),
        8: strip(g_buf, side_out), 9: strip(g_buf, side_in), 10: prior_guest,
    }
    when_recv = {3: has_out, 5: has_in, 7: has_out, 9: has_in}

    def landing(k):
        ref = landed[k]
        return remote(k, ref, ref, a_id)

    def rows_of(k, ref, start, width):
        cols = pl.ds(start, width)
        up = pltpu.make_async_remote_copy(
            src_ref=ref.at[pl.ds(128, 128), cols], dst_ref=ref.at[pl.ds(640, 128), cols],
            send_sem=send_r.at[2 * k], recv_sem=recv_r.at[2 * k], device_id=up_id, device_id_type=MESH,
        )
        down = pltpu.make_async_remote_copy(
            src_ref=ref.at[pl.ds(512, 128), cols], dst_ref=ref.at[pl.ds(0, 128), cols],
            send_sem=send_r.at[2 * k + 1], recv_sem=recv_r.at[2 * k + 1], device_id=down_id, device_id_type=MESH,
        )
        return up, down

    pieces = {
        0: (m_buf, outer_g, 128), 1: (m_buf, near_g, 128), 2: (p_buf, side_in, 128), 3: (p_buf, side_out, 128),
        4: (m_buf, al(c1 + 128), 256), 5: (m_buf, m_far_in, 128), 6: (g_buf, 128, 512), 7: (m_buf, m_far_out, 128),
        8: (g_buf, side_out, 128), 9: (g_buf, side_in, 128), 10: (m_buf, c0, 512), 11: (p_buf, 128, 512),
    }

    def send_rows(k):
        up, down = rows_of(k, *pieces[k])
        pl.when(has_up)(up.start)
        pl.when(has_down)(down.start)

    def wait_rows(k):
        up, down = rows_of(k, *pieces[k])
        pl.when(has_down)(up.wait_recv)
        pl.when(has_up)(down.wait_recv)

    def wait_sent_rows(k):
        up, down = rows_of(k, *pieces[k])
        pl.when(has_up)(up.wait_send)
        pl.when(has_down)(down.wait_send)

    def guarded(k, do):
        if k in when_recv:
            pl.when(when_recv[k])(do)
        else:
            do()

    def arrive(k, forward=None, cond=None):
        def do():
            landing(k).wait_recv()
            send_rows(k)

        guarded(k, do)
        if forward is not None:
            if cond is None:
                forward.start()
            else:
                pl.when(cond)(forward.start)

    send_rows(10)
    send_rows(11)
    landing(10).wait_recv()

    for copy in constants[1:]:
        copy.wait()
    freq, off_u, off_v, mask_v = phases[0:1, :], phases[1:2, :], phases[2:3, :], phases[3:4, :]
    for t in range(2):
        value = prior_own[0] if t == 0 else prior_guest[...]
        sign = (1 - 2 * x_lo) * (1 - 2 * t)
        wide = jnp.concatenate([value] * 4, axis=1) * sign
        turn = wide * freq
        scale = 2.0 * np.pi / PATCH
        u_s[8 * t : 8 * t + 8, :] = jnp.cos(((turn + off_u) & (PATCH - 1)).astype(F32) * scale)
        v_s[8 * t : 8 * t + 8, :] = (
            jnp.cos(((turn + off_v) & (PATCH - 1)).astype(F32) * scale) * mask_v.astype(F32) * sign.astype(F32)
        )

    reach = (lax.broadcasted_iota(jnp.int32, (LAGS, LAGS), 0) - LAGS // 2).astype(F32)
    unit = 1.0 / (512.0 * 512.0 * 512.0)

    def first_pass(src, dst, block):
        at = al(block * 256)
        for i in range(2):
            dst[i, :, pl.ds(at, 256)] = jnp.dot(
                table[...], src[pl.ds(256 * i, 512), pl.ds(at, 256)], preferred_element_type=F32
            ).astype(BF16)

    def rows_in(*ks):
        for k in ks:
            guarded(k, functools.partial(wait_rows, k))

    def lag_table(r):
        return (lag_cos[...] * u_s[pl.ds(r, 1), :] + lag_sin[...] * v_s[pl.ds(r, 1), :]).astype(BF16)

    def pairs(t, j, between=None):
        tile = x_lo if t == 0 else 1 - x_lo
        at_m, at_x = al((tile * 2 + j) * 256), al(j * 256)

        def spectra(h):
            i, kb = h // 2, h % 2
            rows = pl.ds(kb * 256, 256)
            a_s[h % 2] = jnp.dot(zm[i, rows, pl.ds(at_m, 512)], table_t[...], preferred_element_type=F32)
            b_s[h % 2] = jnp.dot(zpg[t, i, rows, pl.ds(at_x, 512)], table_t[...], preferred_element_type=F32)

        def products(h):
            for rc in range(8):
                for lb in range(2):
                    cross_chunk(a_s.at[h % 2], b_s.at[h % 2], mix.at[h // 2], h % 2, lb, rc)

        def window(i):
            n = t * 4 + i * 2 + j
            rows = lag_table(8 * t + i * 2 + j)
            columns = lag_table(8 * t + 4 + i * 2 + j)
            half = jnp.dot(rows, mix[i], preferred_element_type=F32).astype(BF16)
            surface = lax.dot_general(half, columns, (((1,), (1,)), ((), ())), preferred_element_type=F32) * unit
            weights = surface * surface
            sums[0, pl.ds(n, 1), :] = jnp.sum(weights, axis=0, keepdims=True)
            sums[1, pl.ds(n, 1), :] = jnp.sum(weights * reach, axis=0, keepdims=True)

        spectra(0)
        spectra(1)
        products(0)
        spectra(2)
        products(1)
        if between is not None:
            between()
        spectra(3)
        window(0)
        products(2)
        products(3)
        window(1)

    rows_in(10, 11)
    first_pass(m_buf, zm, 1 + 2 * x_lo)
    first_pass(p_buf, zpg.at[0], 1)
    arrive(0, mz_guest, has_in)
    arrive(5)
    hear(0)
    tell(1)
    arrive(1, mb_near)
    rows_in(0, 5)
    first_pass(m_buf, zm, 4 - 4 * x_lo)
    arrive(7, mb_far, has_out)
    hear(1)
    tell(2)
    rows_in(1)
    first_pass(m_buf, zm, 2)
    arrive(2)
    rows_in(7)
    first_pass(m_buf, zm, 4 * x_lo)
    rows_in(2)
    first_pass(p_buf, zpg.at[0], 2 - 2 * x_lo)

    def arrivals():
        arrive(3)
        arrive(6)

    hear(2)
    tell(3)
    pairs(0, 1 - x_lo, arrivals)
    hear(3)
    rows_in(3)
    first_pass(p_buf, zpg.at[0], 2 * x_lo)
    rows_in(6)
    first_pass(g_buf, zpg.at[1], 1)
    pairs(0, x_lo)
    arrive(4)
    arrive(8)
    arrive(9)
    rows_in(4)
    first_pass(m_buf, zm, 3 - 2 * x_lo)
    rows_in(8)
    first_pass(g_buf, zpg.at[1], 2 * x_lo)
    pairs(1, x_lo)
    rows_in(9)
    first_pass(g_buf, zpg.at[1], 2 - 2 * x_lo)
    pairs(1, 1 - x_lo)

    lane = lax.broadcasted_iota(jnp.int32, (8, 128), 1)
    along = (lane - LAGS // 2).astype(F32)
    by_pair = sums[0]
    total = 1.0 + jnp.sum(by_pair, axis=1, keepdims=True)
    shift_r = jnp.sum(sums[1], axis=1, keepdims=True) / total
    shift_c = jnp.sum(by_pair * along, axis=1, keepdims=True) / total

    lane1 = lax.broadcasted_iota(jnp.int32, (1, 128), 1)
    guest_s = 3 - 2 * (gz + x_lo - 2 * gz * x_lo)
    for i in range(2):
        line = jnp.zeros((1, 128), F32)
        for t in range(2):
            s = 2 * gz if t == 0 else guest_s
            c_tile = 2 * z + (x_lo if t == 0 else 1 - x_lo)
            held = prior_own[0] if t == 0 else prior_guest[...]
            for j in range(2):
                n = t * 4 + i * 2 + j
                r = i * 2 + j
                place = s * 16 + 2 * c_tile + j
                flow_r = held[r : r + 1, :].astype(F32) + shift_r[n : n + 1, :]
                flow_c = held[4 + r : 5 + r, :].astype(F32) + shift_c[n : n + 1, :]
                line = line + jnp.where(lane1 == place, flow_r, 0.0) + jnp.where(lane1 == place + 64, flow_c, 0.0)
        flow_send[i : i + 1, :] = line

    n_all = n_gz * n_row * n_col
    me = (gz * n_row + row) * n_col + col
    for dg in range(n_gz):
        for dr in range(n_row):
            for dc in range(n_col):
                if dg or dr or dc:
                    pltpu.make_async_remote_copy(
                        src_ref=flow_send, dst_ref=flow_recv.at[me], send_sem=send_f, recv_sem=recv_f,
                        device_id=at(dg, dr, dc), device_id_type=MESH,
                    ).start()
    want = [row_order[2 * row + m] for m in range(2)]
    picked = [jnp.zeros((1, 128), F32) for _ in range(2)]
    others = flow_recv.at[pl.ds(0, n_all - 1)]
    pltpu.make_async_copy(others, others, recv_f).wait()
    flow_recv[pl.ds(me, 1)] = flow_send[...][None]
    for r in range(n_row):
        block = sum(jnp.sum(flow_recv[pl.ds((g * n_row + r) * n_col, n_col)], axis=0) for g in range(n_gz))
        for m in range(2):
            for i in range(2):
                hit = jnp.full((1, 128), want[m], jnp.int32) == 2 * r + i
                picked[m] = picked[m] + jnp.where(hit, block[i : i + 1, :], 0.0)
    for m in range(2):
        out[m : m + 1, :] = picked[m]
    pltpu.make_async_copy(others, others, send_f).wait()

    sends = [
        (pa_outer, None), (pa_near, None), (m_a, None), (m_n, has_out), (pa_mid, None), (mz_own, has_out), (mb_tile, None),
        (mz_guest, has_in), (mb_near, None), (mb_far, has_out), (prior_send, None),
    ]
    for copy, cond in sends:
        if cond is None:
            copy.wait_send()
        else:
            pl.when(cond)(copy.wait_send)
    for k in range(12):
        guarded(k, functools.partial(wait_sent_rows, k))


def body(sections, priors, row_order):
    table = forward_table()
    lag_cos, lag_sin = lag_tables()
    vmem = pl.BlockSpec(memory_space=pltpu.VMEM)
    dma = pltpu.SemaphoreType.DMA
    return pl.pallas_call(
        kernel,
        out_shape=jax.ShapeDtypeStruct((2, 128), F32),
        in_specs=[pl.BlockSpec(memory_space=pltpu.HBM)] * 8,
        out_specs=vmem,
        scratch_shapes=[
            pltpu.SMEM((2, 2, 2, 2), jnp.int32),
            pltpu.SMEM((16,), jnp.int32),
            pltpu.VMEM((512, 512), BF16),
            pltpu.VMEM((512, 512), BF16),
            pltpu.VMEM((LAGS, 512), F32),
            pltpu.VMEM((LAGS, 512), F32),
            pltpu.VMEM((8, 512), jnp.int32),
            pltpu.VMEM((768, 1280), BF16),
            pltpu.VMEM((2, 768, 768), BF16),
            pltpu.VMEM((2, 512, 1280), BF16),
            pltpu.VMEM((2, 2, 512, 768), BF16),
            pltpu.VMEM((2, 256, 512), F32),
            pltpu.VMEM((2, 256, 512), F32),
            pltpu.VMEM((2, 512, 512), BF16),
            pltpu.VMEM((2, 8, 128), jnp.int32),
            pltpu.VMEM((8, 128), jnp.int32),
            pltpu.VMEM((16, 512), F32),
            pltpu.VMEM((16, 512), F32),
            pltpu.VMEM((2, 8, 128), F32),
            pltpu.VMEM((2, 128), F32),
            pltpu.VMEM((128, 2, 128), F32),
            pltpu.SemaphoreType.REGULAR((4,)),
            dma((9,)),
            dma((11,)),
            dma((11,)),
            dma((24,)),
            dma((24,)),
            dma,
            dma,
        ],
        compiler_params=pltpu.CompilerParams(collective_id=0, has_side_effects=True, vmem_limit_bytes=67_043_328),
    )(
        sections, priors, row_order, jnp.asarray(table), jnp.asarray(np.ascontiguousarray(table.T)),
        jnp.asarray(lag_cos), jnp.asarray(lag_sin), jnp.asarray(phase_rows()),
    )


def solution(mesh):
    return jax.shard_map(
        body,
        mesh=mesh,
        in_specs=(P("gz", "row", "col"), P(None, "gz", "row", "col"), P()),
        out_specs=P("row", None),
        check_vma=False,
    )
```

```python
import functools

import jax
import jax.numpy as jnp
import ml_dtypes
import numpy as np
from jax import lax
from jax.experimental import pallas as pl
from jax.experimental.pallas import tpu as pltpu
from jax.sharding import PartitionSpec as P

PATCH = 512
LAGS = 128
UNIT = 128
MESH = pl.DeviceIdType.MESH
BF16 = jnp.bfloat16
F32 = jnp.float32


def slots():
    m = np.arange(128)
    freq = np.concatenate([2 * m, 2 * m, 2 * m + 1, 2 * m + 1])
    sine = np.concatenate([np.zeros(128), np.ones(128), np.zeros(128), np.ones(128)]).astype(bool)
    weight = np.full(512, 2.0)
    freq[128], sine[128] = 256, False
    weight[0] = weight[128] = 1.0
    return freq, sine, weight


def forward_table():
    freq, sine, _ = slots()
    angle = (freq[:, None] * np.arange(PATCH)[None, :]) % PATCH * (2.0 * np.pi / PATCH)
    return np.where(sine[:, None], np.sin(angle), np.cos(angle)).astype(ml_dtypes.bfloat16)


def lag_tables():
    freq, _, weight = slots()
    lag = np.arange(LAGS) - LAGS // 2
    angle = (freq[None, :] * lag[:, None]) % PATCH * (2.0 * np.pi / PATCH)
    return (np.cos(angle) * weight).astype(np.float32), (np.sin(angle) * weight).astype(np.float32)


def phase_rows():
    freq, sine, _ = slots()
    rows = np.zeros((8, 512), np.int32)
    rows[0] = freq
    rows[1] = np.where(sine, -128, 0)
    rows[2] = np.where(sine, 0, 128)
    rows[3] = 1
    rows[3, 128] = 0
    return rows


def cross_chunk(a, b, m_ref, kb, lb, rc):
    lc, ls = pl.ds(lb * 256, 128), pl.ds(lb * 256 + 128, 128)
    rt, rl = pl.ds(rc * 16, 16), pl.ds(128 + rc * 16, 16)
    mt, ml = pl.ds(kb * 256 + rc * 16, 16), pl.ds(kb * 256 + 128 + rc * 16, 16)
    a1, a2, a3, a4 = a[rt, lc], a[rt, ls], a[rl, lc], a[rl, ls]
    b1, b2, b3, b4 = b[rt, lc], b[rt, ls], b[rl, lc], b[rl, ls]
    p33, p44 = a3 * b3, a4 * b4
    u1, u2 = a1 * b2 - a2 * b1, a3 * b4 - a4 * b3
    v1, v2 = a1 * b3 - a3 * b1, a2 * b4 - a4 * b2
    ss = (a1 * b4 + a4 * b1) - (a2 * b3 + a3 * b2)
    first_row = kb == 0 and rc == 0
    if first_row:
        k0 = lax.broadcasted_iota(jnp.int32, (16, 128), 0) == 0
        z33, z44, zu2 = jnp.where(k0, 0.0, p33), jnp.where(k0, 0.0, p44), jnp.where(k0, 0.0, u2)
    else:
        z33, z44, zu2 = p33, p44, u2
    t1, t2 = a1 * b1 + z33, a2 * b2 + z44
    cc, cs, sc = t1 + t2, u1 + zu2, v1 + v2
    if first_row:
        sc, ss = jnp.where(k0, p33 + p44, sc), jnp.where(k0, u2, ss)
    if lb == 0:
        l0 = lax.broadcasted_iota(jnp.int32, (16, 128), 1) == 0
        cc, cs = jnp.where(l0, t1, cc), jnp.where(l0, t2, cs)
        if first_row:
            sc = jnp.where(l0, jnp.where(k0, p33, v1), sc)
            ss = jnp.where(l0, jnp.where(k0, p44, v2), ss)
        else:
            sc, ss = jnp.where(l0, v1, sc), jnp.where(l0, v2, ss)
    m_ref[mt, lc] = cc.astype(BF16)
    m_ref[mt, ls] = cs.astype(BF16)
    m_ref[ml, lc] = sc.astype(BF16)
    m_ref[ml, ls] = ss.astype(BF16)


def kernel(
    sections, priors_h, row_order_h, table_h, table_t_h, lag_cos_h, lag_sin_h, phases_h, out,
    priors, row_order, table, table_t, lag_cos, lag_sin, phases, m_buf, pg_buf, zm, zpg, a_s, b_s, mix, prior_own, prior_guest, u_s, v_s, lag_s, sums, flow_send, flow_recv, known,
    local_sem, send_x, recv_x, send_r, recv_r, send_f, recv_f,
):
    gz, row, col = lax.axis_index("gz"), lax.axis_index("row"), lax.axis_index("col")
    n_gz, n_row, n_col = lax.axis_size("gz"), lax.axis_size("row"), lax.axis_size("col")
    x_lo = lax.rem(col, 2)
    z = lax.div(col, 2)
    has_left, has_right = z > 0, z < n_col // 2 - 1
    has_out = jnp.logical_or(jnp.logical_and(x_lo == 0, has_left), jnp.logical_and(x_lo == 1, has_right))
    has_in = jnp.logical_or(jnp.logical_and(x_lo == 1, has_left), jnp.logical_and(x_lo == 0, has_right))
    has_up, has_down = row > 0, row < n_row - 1
    side = 2 * x_lo - 1
    a_id = (gz, row, col - side)
    b_id = (1 - gz, row, col - side)
    n_id = (gz, row, col + side)
    z_out = (gz, row, col + 2 * side)
    z_in = (gz, row, col - 2 * side)
    up_id, down_id = (gz, row - 1, col), (gz, row + 1, col)

    def al(v):
        return pl.multiple_of(v, 128)

    c0 = al(128 + 512 * x_lo)
    near, outer = al(512 + 128 * x_lo), al(128 + 896 * x_lo)
    near_p, outer_p = al(512 - 384 * x_lo), al(128 + 384 * x_lo)
    c1 = al(640 - 512 * x_lo)
    near_g, outer_g = al(640 - 128 * x_lo), al(1024 - 896 * x_lo)
    m_far_out, m_far_in = al(1152 * x_lo), al(1152 - 1152 * x_lo)
    side_in, side_out = al(640 - 640 * x_lo), al(640 * x_lo)
    body = pl.ds(128, 512)
    p_buf, g_buf = pg_buf.at[0], pg_buf.at[1]

    own_m = pltpu.make_async_copy(sections.at[x_lo], m_buf.at[body, pl.ds(c0, 512)], local_sem.at[0])
    own_p = pltpu.make_async_copy(sections.at[1 - x_lo], p_buf.at[body, pl.ds(128, 512)], local_sem.at[1])
    own_m.start()
    own_p.start()
    constants = [
        pltpu.make_async_copy(src, dst, local_sem.at[2 + k])
        for k, (src, dst) in enumerate([
            (priors_h, priors), (phases_h, phases), (table_h, table), (table_t_h, table_t),
            (lag_cos_h, lag_cos), (lag_sin_h, lag_sin), (row_order_h, row_order),
        ])
    ]
    for copy in constants:
        copy.start()

    def at(dg, dr, dc):
        return (lax.rem(gz + dg, n_gz), lax.rem(row + dr, n_row), lax.rem(col + dc, n_col))

    z_ring = [at(0, 0, 2), at(0, 0, n_col - 2)]
    row_ring = [at(0, 1, 0), at(0, n_row - 1, 0)]
    near_peers = [a_id, b_id] + z_ring + row_ring
    barrier = pltpu.get_barrier_semaphore()
    for peer in near_peers:
        pl.semaphore_signal(barrier, inc=1, device_id=peer, device_id_type=MESH)

    rounds = [
        near_peers,
        [a_id, b_id, (1 - gz, row, col)],
        z_ring + [at(0, 0, n_col // 2)],
        [at(0, 2, 0), at(0, n_row - 2, 0)],
    ]

    def tell(k):
        for peer in rounds[k]:
            pl.semaphore_signal(known.at[k], inc=1, device_id=peer, device_id_type=MESH)

    def hear(k):
        pl.semaphore_wait(known.at[k], len(rounds[k]))

    constants[0].wait()
    for c in range(2):
        for ii in range(2):
            for jj in range(2):
                r = c * 4 + ii * 2 + jj
                prior_own[0, r : r + 1, :] = jnp.full((1, 128), priors[c, 0, ii, jj], jnp.int32)
                prior_own[1, r : r + 1, :] = jnp.full((1, 128), priors[c, 1, ii, jj], jnp.int32)

    @pl.when(row == 0)
    def _():
        m_buf[0:128, :] = jnp.zeros((128, 1280), BF16)
        pg_buf[:, 0:128, :] = jnp.zeros((2, 128, 768), BF16)

    @pl.when(row == n_row - 1)
    def _():
        m_buf[640:768, :] = jnp.zeros((128, 1280), BF16)
        pg_buf[:, 640:768, :] = jnp.zeros((2, 128, 768), BF16)

    @pl.when(jnp.logical_not(has_left))
    def _():
        m_buf[:, 0:128] = jnp.zeros((768, 128), BF16)
        pg_buf[x_lo, :, 0:128] = jnp.zeros((768, 128), BF16)

    @pl.when(jnp.logical_not(has_right))
    def _():
        m_buf[:, 1152:1280] = jnp.zeros((768, 128), BF16)
        pg_buf[1 - x_lo, :, 640:768] = jnp.zeros((768, 128), BF16)

    own_m.wait()
    own_p.wait()
    pl.semaphore_wait(barrier, len(near_peers))
    tell(0)

    spans = (pl.ds(128, 128), pl.ds(512, 128), pl.ds(256, 256))

    def part(k, p, src, src_at, dst, dst_at, width, device):
        return pltpu.make_async_remote_copy(
            src_ref=src.at[spans[p], pl.ds(src_at, width)], dst_ref=dst.at[spans[p], pl.ds(dst_at, width)],
            send_sem=send_x.at[3 * k + p], recv_sem=recv_x.at[3 * k + p], device_id=device, device_id_type=MESH,
        )

    sent = {
        0: (p_buf, outer_p, m_buf, outer, 128, a_id),
        1: (p_buf, near_p, m_buf, near, 128, a_id),
        2: (m_buf, near, p_buf, side_out, 128, a_id),
        3: (m_buf, outer, p_buf, side_in, 128, n_id),
        4: (p_buf, 256, m_buf, al(c0 + 128), 256, a_id),
        5: (m_buf, outer, m_buf, m_far_in, 128, z_out),
        6: (m_buf, c0, g_buf, 128, 512, b_id),
        7: (m_buf, outer_g, m_buf, m_far_out, 128, z_in),
        8: (m_buf, near_g, g_buf, side_in, 128, b_id),
        9: (m_buf, m_far_out, g_buf, side_out, 128, b_id),
        10: (m_buf, c0, g_buf, 128, 256, b_id),
        11: (m_buf, al(c0 + 256), g_buf, 384, 256, b_id),
    }
    landed = {
        0: (m_buf, outer_g, 128), 1: (m_buf, near_g, 128), 2: (p_buf, side_in, 128), 3: (p_buf, side_out, 128),
        4: (m_buf, al(c1 + 128), 256), 5: (m_buf, m_far_in, 128), 6: (g_buf, 128, 512), 7: (m_buf, m_far_out, 128),
        8: (g_buf, side_out, 128), 9: (g_buf, side_in, 128), 10: (g_buf, 128, 256), 11: (g_buf, 384, 256),
    }
    parts_of = {k: (0, 1, 2) for k in range(10)}
    parts_of.update({6: (0, 1), 10: (2,), 11: (2,)})
    when_send = {3: has_out, 5: has_out, 7: has_in, 9: has_out}
    when_recv = {3: has_out, 5: has_in, 7: has_out, 9: has_in}

    def guarded(conds, k, do):
        if k in conds:
            pl.when(conds[k])(do)
        else:
            do()

    def send(k, *parts):
        def do():
            for p in parts:
                part(k, p, *sent[k]).start()

        guarded(when_send, k, do)

    def land(k, p):
        ref, start, width = landed[k]
        part(k, p, ref, start, ref, start, width, a_id).wait_recv()

    pieces = dict(landed)
    pieces.update({10: (m_buf, c0, 512), 11: (p_buf, 128, 512)})

    def row_copy(k, down):
        ref, start, width = pieces[k]
        cols = pl.ds(start, width)
        src, dst = (pl.ds(512, 128), pl.ds(0, 128)) if down else (pl.ds(128, 128), pl.ds(640, 128))
        return pltpu.make_async_remote_copy(
            src_ref=ref.at[src, cols], dst_ref=ref.at[dst, cols], send_sem=send_r.at[2 * k + down],
            recv_sem=recv_r.at[2 * k + down], device_id=down_id if down else up_id, device_id_type=MESH,
        )

    def send_row(k, down):
        pl.when(has_down if down else has_up)(row_copy(k, down).start)

    def edges(k, forward=None):
        def do():
            for p in range(2):
                land(k, p)
                send_row(k, p)

        guarded(when_recv, k, do)
        if forward is not None:
            send(forward, 0, 1)

    def centre(k, forward=None):
        guarded(when_recv, k, lambda: land(k, 2))
        if forward is not None:
            send(forward, 2)

    def rows_in(*ks):
        def do(k):
            pl.when(has_down)(row_copy(k, 0).wait_recv)
            pl.when(has_up)(row_copy(k, 1).wait_recv)

        for k in ks:
            guarded(when_recv, k, functools.partial(do, k))

    prior_id = (gz + x_lo * (1 - 2 * gz), row, col - side)
    prior_send = pltpu.make_async_remote_copy(
        src_ref=prior_own.at[1], dst_ref=prior_guest, send_sem=send_x.at[36], recv_sem=recv_x.at[36],
        device_id=prior_id, device_id_type=MESH,
    )

    send(0, 0, 1)
    send(6, 0, 1)
    send(5, 0, 1)
    send(0, 2)
    send(1, 0, 1)
    send(5, 2)
    send(1, 2)
    send(10, 2)
    send(2, 0, 1, 2)
    prior_send.start()
    for k in (10, 11):
        for down in range(2):
            send_row(k, down)

    for copy in constants[1:]:
        copy.wait()
    freq, off_u, off_v, mask_v = phases[0:1, :], phases[1:2, :], phases[2:3, :], phases[3:4, :]

    def lag_tables_of(t):
        value = prior_own[0] if t == 0 else prior_guest[...]
        sign = (1 - 2 * x_lo) * (1 - 2 * t)
        turn = jnp.concatenate([value] * 4, axis=1) * sign * freq
        scale = 2.0 * np.pi / PATCH
        u_s[...] = jnp.cos(((turn + off_u) & (PATCH - 1)).astype(F32) * scale)
        v_s[...] = jnp.cos(((turn + off_v) & (PATCH - 1)).astype(F32) * scale) * mask_v.astype(F32) * sign.astype(F32)

        @pl.loop(0, 8)
        def _(r):
            lag_s[8 * t + r] = (lag_cos[...] * u_s[pl.ds(r, 1), :] + lag_sin[...] * v_s[pl.ds(r, 1), :]).astype(BF16)

    reach = (lax.broadcasted_iota(jnp.int32, (LAGS, LAGS), 0) - LAGS // 2).astype(F32)
    unit = 1.0 / (512.0 * 512.0 * 512.0)

    def first_pass(src, dst, block):
        at = al(block * 256)
        for i in range(2):
            dst[i, :, pl.ds(at, 256)] = jnp.dot(
                table[...], src[pl.ds(256 * i, 512), pl.ds(at, 256)], preferred_element_type=F32
            ).astype(BF16)

    def pairs(t, j, between=None, b_done=False):
        tile = x_lo if t == 0 else 1 - x_lo
        at_m = al((tile * 2 + j) * 256)

        def spectra(h):
            i, kb = h // 2, h % 2
            a_s[h % 2] = jnp.dot(zm[i, pl.ds(kb * 256, 256), pl.ds(at_m, 512)], table_t[...], preferred_element_type=F32)
            if not b_done:
                spectra_b(t, j, h)

        def products(h):
            for rc in range(8):
                for lb in range(2):
                    cross_chunk(a_s.at[h % 2], b_s.at[h], mix.at[h // 2], h % 2, lb, rc)

        def window(i):
            n = t * 4 + i * 2 + j
            half = jnp.dot(lag_s[8 * t + i * 2 + j], mix[i], preferred_element_type=F32).astype(BF16)
            surface = unit * lax.dot_general(
                half, lag_s[8 * t + 4 + i * 2 + j], (((1,), (1,)), ((), ())), preferred_element_type=F32
            )
            weights = surface * surface
            sums[0, pl.ds(n, 1), :] = jnp.sum(weights, axis=0, keepdims=True)
            sums[1, pl.ds(n, 1), :] = jnp.sum(weights * reach, axis=0, keepdims=True)

        spectra(0)
        spectra(1)
        products(0)
        spectra(2)
        products(1)
        if between is not None:
            between()
        spectra(3)
        window(0)
        products(2)
        products(3)
        window(1)

    def spectra_b(t, j, h):
        b_s[h] = jnp.dot(
            zpg[t, h // 2, pl.ds(h % 2 * 256, 256), pl.ds(al(j * 256), 512)], table_t[...], preferred_element_type=F32
        )

    hear(0)
    send(3, 0, 1, 2)
    send(4, 0, 1, 2)
    tell(1)
    lag_tables_of(0)
    edges(0, 7)
    rows_in(10)
    first_pass(m_buf, zm, 1 + 2 * x_lo)
    centre(0, 7)
    edges(5)
    edges(1, 8)
    edges(7, 9)
    send(11, 2)
    rows_in(11)
    first_pass(p_buf, zpg.at[0], 1)
    centre(1, 8)
    prior_send.wait_recv()
    lag_tables_of(1)
    centre(5)
    rows_in(0, 5)
    first_pass(m_buf, zm, 4 - 4 * x_lo)
    centre(7, 9)
    hear(1)
    tell(2)
    rows_in(1)
    first_pass(m_buf, zm, 2)
    edges(2)
    rows_in(7)
    first_pass(m_buf, zm, 4 * x_lo)
    centre(2)
    rows_in(2)
    first_pass(p_buf, zpg.at[0], 2 - 2 * x_lo)
    hear(2)
    tell(3)

    def arrivals():
        edges(3)
        edges(6)

    pairs(0, 1 - x_lo, arrivals)
    hear(3)
    centre(3)
    rows_in(3)
    first_pass(p_buf, zpg.at[0], 2 * x_lo)
    edges(8)
    pairs(0, x_lo)
    edges(9)
    edges(4)
    centre(10)
    centre(11)
    rows_in(6)
    first_pass(g_buf, zpg.at[1], 1)
    centre(8)
    rows_in(8)
    first_pass(g_buf, zpg.at[1], 2 * x_lo)
    for h in range(4):
        spectra_b(1, x_lo, h)
    centre(4)
    rows_in(4)
    first_pass(m_buf, zm, 3 - 2 * x_lo)
    pairs(1, x_lo, b_done=True)
    centre(9)
    rows_in(9)
    first_pass(g_buf, zpg.at[1], 2 - 2 * x_lo)
    pairs(1, 1 - x_lo)

    lane = lax.broadcasted_iota(jnp.int32, (8, 128), 1)
    along = (lane - LAGS // 2).astype(F32)
    by_pair = sums[0]
    total = 1.0 + jnp.sum(by_pair, axis=1, keepdims=True)
    shift_r = jnp.sum(sums[1], axis=1, keepdims=True) / total
    shift_c = jnp.sum(by_pair * along, axis=1, keepdims=True) / total

    lane1 = lax.broadcasted_iota(jnp.int32, (1, 128), 1)
    guest_s = 3 - 2 * (gz + x_lo - 2 * gz * x_lo)
    for i in range(2):
        line = jnp.zeros((1, 128), F32)
        for t in range(2):
            s = 2 * gz if t == 0 else guest_s
            c_tile = 2 * z + (x_lo if t == 0 else 1 - x_lo)
            held = prior_own[0] if t == 0 else prior_guest[...]
            for j in range(2):
                n = t * 4 + i * 2 + j
                r = i * 2 + j
                place = s * 16 + 2 * c_tile + j
                flow_r = held[r : r + 1, :].astype(F32) + shift_r[n : n + 1, :]
                flow_c = held[4 + r : 5 + r, :].astype(F32) + shift_c[n : n + 1, :]
                line = line + jnp.where(lane1 == place, flow_r, 0.0) + jnp.where(lane1 == place + 64, flow_c, 0.0)
        flow_send[i : i + 1, :] = line

    n_all = n_gz * n_row * n_col
    me = (gz * n_row + row) * n_col + col
    for dg in range(n_gz):
        for dr in range(n_row):
            for dc in range(n_col):
                if dg or dr or dc:
                    pltpu.make_async_remote_copy(
                        src_ref=flow_send, dst_ref=flow_recv.at[me], send_sem=send_f, recv_sem=recv_f,
                        device_id=at(dg, dr, dc), device_id_type=MESH,
                    ).start()
    want = [row_order[2 * row + m] for m in range(2)]
    picked = [jnp.zeros((1, 128), F32) for _ in range(2)]
    others = flow_recv.at[pl.ds(0, n_all - 1)]
    pltpu.make_async_copy(others, others, recv_f).wait()
    flow_recv[pl.ds(me, 1)] = flow_send[...][None]
    for r in range(n_row):
        block = sum(jnp.sum(flow_recv[pl.ds((g * n_row + r) * n_col, n_col)], axis=0) for g in range(n_gz))
        for m in range(2):
            for i in range(2):
                hit = jnp.full((1, 128), want[m], jnp.int32) == 2 * r + i
                picked[m] = picked[m] + jnp.where(hit, block[i : i + 1, :], 0.0)
    for m in range(2):
        out[m : m + 1, :] = picked[m]
    pltpu.make_async_copy(others, others, send_f).wait()

    prior_send.wait_send()
    for k in range(12):
        def sent_all(k=k):
            for p in parts_of[k]:
                part(k, p, *sent[k]).wait_send()

        guarded(when_send, k, sent_all)

        def rows_sent(k=k):
            pl.when(has_up)(row_copy(k, 0).wait_send)
            pl.when(has_down)(row_copy(k, 1).wait_send)

        guarded(when_recv, k, rows_sent)


def body(sections, priors, row_order):
    table = forward_table()
    lag_cos, lag_sin = lag_tables()
    vmem = pl.BlockSpec(memory_space=pltpu.VMEM)
    dma = pltpu.SemaphoreType.DMA
    return pl.pallas_call(
        kernel,
        out_shape=jax.ShapeDtypeStruct((2, 128), F32),
        in_specs=[pl.BlockSpec(memory_space=pltpu.HBM)] * 8,
        out_specs=vmem,
        scratch_shapes=[
            pltpu.SMEM((2, 2, 2, 2), jnp.int32),
            pltpu.SMEM((16,), jnp.int32),
            pltpu.VMEM((512, 512), BF16),
            pltpu.VMEM((512, 512), BF16),
            pltpu.VMEM((LAGS, 512), F32),
            pltpu.VMEM((LAGS, 512), F32),
            pltpu.VMEM((8, 512), jnp.int32),
            pltpu.VMEM((768, 1280), BF16),
            pltpu.VMEM((2, 768, 768), BF16),
            pltpu.VMEM((2, 512, 1280), BF16),
            pltpu.VMEM((2, 2, 512, 768), BF16),
            pltpu.VMEM((2, 256, 512), F32),
            pltpu.VMEM((4, 256, 512), F32),
            pltpu.VMEM((2, 512, 512), BF16),
            pltpu.VMEM((2, 8, 128), jnp.int32),
            pltpu.VMEM((8, 128), jnp.int32),
            pltpu.VMEM((8, 512), F32),
            pltpu.VMEM((8, 512), F32),
            pltpu.VMEM((16, LAGS, 512), BF16),
            pltpu.VMEM((2, 8, 128), F32),
            pltpu.VMEM((2, 128), F32),
            pltpu.VMEM((128, 2, 128), F32),
            pltpu.SemaphoreType.REGULAR((4,)),
            dma((9,)),
            dma((37,)),
            dma((37,)),
            dma((24,)),
            dma((24,)),
            dma,
            dma,
        ],
        compiler_params=pltpu.CompilerParams(collective_id=0, has_side_effects=True, vmem_limit_bytes=67_043_328),
    )(
        sections, priors, row_order, jnp.asarray(table), jnp.asarray(np.ascontiguousarray(table.T)),
        jnp.asarray(lag_cos), jnp.asarray(lag_sin), jnp.asarray(phase_rows()),
    )


def solution(mesh):
    return jax.shard_map(
        body,
        mesh=mesh,
        in_specs=(P("gz", "row", "col"), P(None, "gz", "row", "col"), P()),
        out_specs=P("row", None),
        check_vma=False,
    )
```

```python
import functools

import jax
import jax.numpy as jnp
import ml_dtypes
import numpy as np
from jax import lax
from jax.experimental import pallas as pl
from jax.experimental.pallas import tpu as pltpu
from jax.sharding import PartitionSpec as P

PATCH = 512
LAGS = 128
UNIT = 128
MESH = pl.DeviceIdType.MESH
BF16 = jnp.bfloat16
F32 = jnp.float32


def slots():
    m = np.arange(128)
    freq = np.concatenate([2 * m, 2 * m, 2 * m + 1, 2 * m + 1])
    sine = np.concatenate([np.zeros(128), np.ones(128), np.zeros(128), np.ones(128)]).astype(bool)
    weight = np.full(512, 2.0)
    freq[128], sine[128] = 256, False
    weight[0] = weight[128] = 1.0
    return freq, sine, weight


def forward_table():
    freq, sine, _ = slots()
    angle = (freq[:, None] * np.arange(PATCH)[None, :]) % PATCH * (2.0 * np.pi / PATCH)
    return np.where(sine[:, None], np.sin(angle), np.cos(angle)).astype(ml_dtypes.bfloat16)


def lag_tables():
    freq, _, weight = slots()
    lag = np.arange(LAGS) - LAGS // 2
    angle = (freq[None, :] * lag[:, None]) % PATCH * (2.0 * np.pi / PATCH)
    return (np.cos(angle) * weight).astype(np.float32), (np.sin(angle) * weight).astype(np.float32)


def phase_rows():
    freq, sine, _ = slots()
    rows = np.zeros((8, 512), np.int32)
    rows[0] = freq
    rows[1] = np.where(sine, -128, 0)
    rows[2] = np.where(sine, 0, 128)
    rows[3] = 1
    rows[3, 128] = 0
    return rows


def cross_chunk(a, b, m_ref, kb, lb, rc):
    lc, ls = pl.ds(lb * 256, 128), pl.ds(lb * 256 + 128, 128)
    rt, rl = pl.ds(rc * 16, 16), pl.ds(128 + rc * 16, 16)
    mt, ml = pl.ds(kb * 256 + rc * 16, 16), pl.ds(kb * 256 + 128 + rc * 16, 16)
    a1, a2, a3, a4 = a[rt, lc], a[rt, ls], a[rl, lc], a[rl, ls]
    b1, b2, b3, b4 = b[rt, lc], b[rt, ls], b[rl, lc], b[rl, ls]
    p33, p44 = a3 * b3, a4 * b4
    u1, u2 = a1 * b2 - a2 * b1, a3 * b4 - a4 * b3
    v1, v2 = a1 * b3 - a3 * b1, a2 * b4 - a4 * b2
    ss = (a1 * b4 + a4 * b1) - (a2 * b3 + a3 * b2)
    first_row = kb == 0 and rc == 0
    if first_row:
        k0 = lax.broadcasted_iota(jnp.int32, (16, 128), 0) == 0
        z33, z44, zu2 = jnp.where(k0, 0.0, p33), jnp.where(k0, 0.0, p44), jnp.where(k0, 0.0, u2)
    else:
        z33, z44, zu2 = p33, p44, u2
    t1, t2 = a1 * b1 + z33, a2 * b2 + z44
    cc, cs, sc = t1 + t2, u1 + zu2, v1 + v2
    if first_row:
        sc, ss = jnp.where(k0, p33 + p44, sc), jnp.where(k0, u2, ss)
    if lb == 0:
        l0 = lax.broadcasted_iota(jnp.int32, (16, 128), 1) == 0
        cc, cs = jnp.where(l0, t1, cc), jnp.where(l0, t2, cs)
        if first_row:
            sc = jnp.where(l0, jnp.where(k0, p33, v1), sc)
            ss = jnp.where(l0, jnp.where(k0, p44, v2), ss)
        else:
            sc, ss = jnp.where(l0, v1, sc), jnp.where(l0, v2, ss)
    m_ref[mt, lc] = cc.astype(BF16)
    m_ref[mt, ls] = cs.astype(BF16)
    m_ref[ml, lc] = sc.astype(BF16)
    m_ref[ml, ls] = ss.astype(BF16)


def kernel(
    sections, priors_h, row_order_h, table_h, table_t_h, lag_cos_h, lag_sin_h, phases_h, out,
    priors, row_order, table, table_t, lag_cos, lag_sin, phases, m_buf, pg_buf, zm, zpg, a_s, b_s, mix, prior_own, prior_guest, u_s, v_s, lag_s, sums, flow_send, flow_recv, known,
    local_sem, send_x, recv_x, send_r, recv_r, send_f, recv_f,
):
    gz, row, col = lax.axis_index("gz"), lax.axis_index("row"), lax.axis_index("col")
    n_gz, n_row, n_col = lax.axis_size("gz"), lax.axis_size("row"), lax.axis_size("col")
    x_lo = lax.rem(col, 2)
    z = lax.div(col, 2)
    has_left, has_right = z > 0, z < n_col // 2 - 1
    has_out = jnp.logical_or(jnp.logical_and(x_lo == 0, has_left), jnp.logical_and(x_lo == 1, has_right))
    has_in = jnp.logical_or(jnp.logical_and(x_lo == 1, has_left), jnp.logical_and(x_lo == 0, has_right))
    has_up, has_down = row > 0, row < n_row - 1
    side = 2 * x_lo - 1
    a_id = (gz, row, col - side)
    b_id = (1 - gz, row, col - side)
    n_id = (gz, row, col + side)
    z_out = (gz, row, col + 2 * side)
    z_in = (gz, row, col - 2 * side)
    up_id, down_id = (gz, row - 1, col), (gz, row + 1, col)

    def al(v):
        return pl.multiple_of(v, 128)

    c0 = al(128 + 512 * x_lo)
    near, outer = al(512 + 128 * x_lo), al(128 + 896 * x_lo)
    near_p, outer_p = al(512 - 384 * x_lo), al(128 + 384 * x_lo)
    c1 = al(640 - 512 * x_lo)
    near_g, outer_g = al(640 - 128 * x_lo), al(1024 - 896 * x_lo)
    m_far_out, m_far_in = al(1152 * x_lo), al(1152 - 1152 * x_lo)
    side_in, side_out = al(640 - 640 * x_lo), al(640 * x_lo)
    body = pl.ds(128, 512)
    p_buf, g_buf = pg_buf.at[0], pg_buf.at[1]

    own_m = pltpu.make_async_copy(sections.at[x_lo], m_buf.at[body, pl.ds(c0, 512)], local_sem.at[0])
    own_p = pltpu.make_async_copy(sections.at[1 - x_lo], p_buf.at[body, pl.ds(128, 512)], local_sem.at[1])
    own_m.start()
    own_p.start()
    constants = [
        pltpu.make_async_copy(src, dst, local_sem.at[2 + k])
        for k, (src, dst) in enumerate([
            (priors_h, priors), (phases_h, phases), (table_h, table), (table_t_h, table_t),
            (lag_cos_h, lag_cos), (lag_sin_h, lag_sin), (row_order_h, row_order),
        ])
    ]
    for copy in constants:
        copy.start()

    def at(dg, dr, dc):
        return (lax.rem(gz + dg, n_gz), lax.rem(row + dr, n_row), lax.rem(col + dc, n_col))

    z_ring = [at(0, 0, 2), at(0, 0, n_col - 2)]
    row_ring = [at(0, 1, 0), at(0, n_row - 1, 0)]
    near_peers = [a_id, b_id] + z_ring + row_ring
    barrier = pltpu.get_barrier_semaphore()
    for peer in near_peers:
        pl.semaphore_signal(barrier, inc=1, device_id=peer, device_id_type=MESH)

    rounds = [
        near_peers,
        [a_id, b_id, (1 - gz, row, col)],
        z_ring + [at(0, 0, n_col // 2)],
        [at(0, 2, 0), at(0, n_row - 2, 0)],
    ]

    def tell(k):
        for peer in rounds[k]:
            pl.semaphore_signal(known.at[k], inc=1, device_id=peer, device_id_type=MESH)

    def hear(k):
        pl.semaphore_wait(known.at[k], len(rounds[k]))

    constants[0].wait()
    for c in range(2):
        for ii in range(2):
            for jj in range(2):
                r = c * 4 + ii * 2 + jj
                prior_own[0, r : r + 1, :] = jnp.full((1, 128), priors[c, 0, ii, jj], jnp.int32)
                prior_own[1, r : r + 1, :] = jnp.full((1, 128), priors[c, 1, ii, jj], jnp.int32)

    @pl.when(row == 0)
    def _():
        m_buf[0:128, :] = jnp.zeros((128, 1280), BF16)
        pg_buf[:, 0:128, :] = jnp.zeros((2, 128, 768), BF16)

    @pl.when(row == n_row - 1)
    def _():
        m_buf[640:768, :] = jnp.zeros((128, 1280), BF16)
        pg_buf[:, 640:768, :] = jnp.zeros((2, 128, 768), BF16)

    @pl.when(jnp.logical_not(has_left))
    def _():
        m_buf[:, 0:128] = jnp.zeros((768, 128), BF16)
        pg_buf[x_lo, :, 0:128] = jnp.zeros((768, 128), BF16)

    @pl.when(jnp.logical_not(has_right))
    def _():
        m_buf[:, 1152:1280] = jnp.zeros((768, 128), BF16)
        pg_buf[1 - x_lo, :, 640:768] = jnp.zeros((768, 128), BF16)

    own_m.wait()
    own_p.wait()
    pl.semaphore_wait(barrier, len(near_peers))
    tell(0)

    spans = (pl.ds(128, 128), pl.ds(512, 128), pl.ds(256, 256))

    def part(k, p, src, src_at, dst, dst_at, width, device):
        return pltpu.make_async_remote_copy(
            src_ref=src.at[spans[p], pl.ds(src_at, width)], dst_ref=dst.at[spans[p], pl.ds(dst_at, width)],
            send_sem=send_x.at[3 * k + p], recv_sem=recv_x.at[3 * k + p], device_id=device, device_id_type=MESH,
        )

    sent = {
        0: (p_buf, outer_p, m_buf, outer, 128, a_id),
        1: (p_buf, near_p, m_buf, near, 128, a_id),
        2: (m_buf, near, p_buf, side_out, 128, a_id),
        3: (m_buf, outer, p_buf, side_in, 128, n_id),
        4: (p_buf, 256, m_buf, al(c0 + 128), 256, a_id),
        5: (m_buf, outer, m_buf, m_far_in, 128, z_out),
        6: (m_buf, c0, g_buf, 128, 512, b_id),
        7: (m_buf, outer_g, m_buf, m_far_out, 128, z_in),
        8: (m_buf, near_g, g_buf, side_in, 128, b_id),
        9: (m_buf, m_far_out, g_buf, side_out, 128, b_id),
        10: (m_buf, c0, g_buf, 128, 256, b_id),
        11: (m_buf, al(c0 + 256), g_buf, 384, 256, b_id),
    }
    landed = {
        0: (m_buf, outer_g, 128), 1: (m_buf, near_g, 128), 2: (p_buf, side_in, 128), 3: (p_buf, side_out, 128),
        4: (m_buf, al(c1 + 128), 256), 5: (m_buf, m_far_in, 128), 6: (g_buf, 128, 512), 7: (m_buf, m_far_out, 128),
        8: (g_buf, side_out, 128), 9: (g_buf, side_in, 128), 10: (g_buf, 128, 256), 11: (g_buf, 384, 256),
    }
    parts_of = {k: (0, 1, 2) for k in range(10)}
    parts_of.update({6: (0, 1), 10: (2,), 11: (2,)})
    when_send = {3: has_out, 5: has_out, 7: has_in, 9: has_out}
    when_recv = {3: has_out, 5: has_in, 7: has_out, 9: has_in}

    def guarded(conds, k, do):
        if k in conds:
            pl.when(conds[k])(do)
        else:
            do()

    def send(k, *parts):
        def do():
            for p in parts:
                part(k, p, *sent[k]).start()

        guarded(when_send, k, do)

    def land(k, p):
        ref, start, width = landed[k]
        part(k, p, ref, start, ref, start, width, a_id).wait_recv()

    pieces = dict(landed)
    pieces.update({10: (m_buf, c0, 512), 11: (p_buf, 128, 512)})

    def row_copy(k, down):
        ref, start, width = pieces[k]
        cols = pl.ds(start, width)
        src, dst = (pl.ds(512, 128), pl.ds(0, 128)) if down else (pl.ds(128, 128), pl.ds(640, 128))
        return pltpu.make_async_remote_copy(
            src_ref=ref.at[src, cols], dst_ref=ref.at[dst, cols], send_sem=send_r.at[2 * k + down],
            recv_sem=recv_r.at[2 * k + down], device_id=down_id if down else up_id, device_id_type=MESH,
        )

    def send_row(k, down):
        pl.when(has_down if down else has_up)(row_copy(k, down).start)

    def edges(k, forward=None):
        def do():
            for p in range(2):
                land(k, p)
                send_row(k, p)

        guarded(when_recv, k, do)
        if forward is not None:
            send(forward, 0, 1)

    def centre(k, forward=None):
        guarded(when_recv, k, lambda: land(k, 2))
        if forward is not None:
            send(forward, 2)

    def rows_in(*ks):
        def do(k):
            pl.when(has_down)(row_copy(k, 0).wait_recv)
            pl.when(has_up)(row_copy(k, 1).wait_recv)

        for k in ks:
            guarded(when_recv, k, functools.partial(do, k))

    prior_id = (gz + x_lo * (1 - 2 * gz), row, col - side)
    prior_send = pltpu.make_async_remote_copy(
        src_ref=prior_own.at[1], dst_ref=prior_guest, send_sem=send_x.at[36], recv_sem=recv_x.at[36],
        device_id=prior_id, device_id_type=MESH,
    )

    prior_send.start()
    send(0, 0, 1)
    send(6, 0, 1)
    send(5, 0, 1)
    send(0, 2)
    send(1, 0, 1)
    send(5, 2)
    send(1, 2)
    send(10, 2)
    send(2, 0, 1, 2)
    for k in (10, 11):
        for down in range(2):
            send_row(k, down)

    for copy in constants[1:]:
        copy.wait()
    freq, off_u, off_v, mask_v = phases[0:1, :], phases[1:2, :], phases[2:3, :], phases[3:4, :]

    def lag_tables_of(t):
        value = prior_own[0] if t == 0 else prior_guest[...]
        sign = (1 - 2 * x_lo) * (1 - 2 * t)
        turn = jnp.concatenate([value] * 4, axis=1) * sign * freq
        scale = 2.0 * np.pi / PATCH
        u_s[...] = jnp.cos(((turn + off_u) & (PATCH - 1)).astype(F32) * scale)
        v_s[...] = jnp.cos(((turn + off_v) & (PATCH - 1)).astype(F32) * scale) * mask_v.astype(F32) * sign.astype(F32)

        @pl.loop(0, 8)
        def _(r):
            lag_s[8 * t + r] = (lag_cos[...] * u_s[pl.ds(r, 1), :] + lag_sin[...] * v_s[pl.ds(r, 1), :]).astype(BF16)

    reach = (lax.broadcasted_iota(jnp.int32, (LAGS, LAGS), 0) - LAGS // 2).astype(F32)
    unit = 1.0 / (512.0 * 512.0 * 512.0)

    def first_pass(src, dst, block):
        at = al(block * 256)
        for i in range(2):
            dst[i, :, pl.ds(at, 256)] = jnp.dot(
                table[...], src[pl.ds(256 * i, 512), pl.ds(at, 256)], preferred_element_type=F32
            ).astype(BF16)

    def pairs(t, j, between=None, b_done=False):
        tile = x_lo if t == 0 else 1 - x_lo
        at_m = al((tile * 2 + j) * 256)

        def spectra(h):
            i, kb = h // 2, h % 2
            a_s[h % 2] = jnp.dot(zm[i, pl.ds(kb * 256, 256), pl.ds(at_m, 512)], table_t[...], preferred_element_type=F32)
            if not b_done:
                spectra_b(t, j, h)

        def products(h):
            for rc in range(8):
                for lb in range(2):
                    cross_chunk(a_s.at[h % 2], b_s.at[h], mix.at[h // 2], h % 2, lb, rc)

        def window(i):
            n = t * 4 + i * 2 + j
            half = jnp.dot(lag_s[8 * t + i * 2 + j], mix[i], preferred_element_type=F32).astype(BF16)
            surface = unit * lax.dot_general(
                half, lag_s[8 * t + 4 + i * 2 + j], (((1,), (1,)), ((), ())), preferred_element_type=F32
            )
            weights = surface * surface
            sums[0, pl.ds(n, 1), :] = jnp.sum(weights, axis=0, keepdims=True)
            sums[1, pl.ds(n, 1), :] = jnp.sum(weights * reach, axis=0, keepdims=True)

        spectra(0)
        spectra(1)
        products(0)
        spectra(2)
        products(1)
        if between is not None:
            between()
        spectra(3)
        window(0)
        products(2)
        products(3)
        window(1)

    def spectra_b(t, j, h):
        b_s[h] = jnp.dot(
            zpg[t, h // 2, pl.ds(h % 2 * 256, 256), pl.ds(al(j * 256), 512)], table_t[...], preferred_element_type=F32
        )

    hear(0)
    send(3, 0, 1, 2)
    send(4, 0, 1, 2)
    tell(1)
    lag_tables_of(0)
    edges(0, 7)
    rows_in(10)
    first_pass(m_buf, zm, 1 + 2 * x_lo)
    centre(0, 7)
    edges(5)
    edges(1, 8)
    edges(7, 9)
    send(11, 2)
    rows_in(11)
    first_pass(p_buf, zpg.at[0], 1)
    centre(1, 8)
    prior_send.wait_recv()
    lag_tables_of(1)
    centre(5)
    rows_in(0, 5)
    first_pass(m_buf, zm, 4 - 4 * x_lo)
    centre(7, 9)
    hear(1)
    tell(2)
    rows_in(1)
    first_pass(m_buf, zm, 2)
    edges(2)
    rows_in(7)
    first_pass(m_buf, zm, 4 * x_lo)
    centre(2)
    rows_in(2)
    first_pass(p_buf, zpg.at[0], 2 - 2 * x_lo)
    hear(2)
    tell(3)

    def arrivals():
        edges(3)
        edges(6)

    pairs(0, 1 - x_lo, arrivals)
    hear(3)
    centre(3)
    rows_in(3)
    first_pass(p_buf, zpg.at[0], 2 * x_lo)
    edges(8)
    edges(9)
    pairs(0, x_lo, lambda: edges(4))
    centre(10)
    centre(11)
    rows_in(6)
    first_pass(g_buf, zpg.at[1], 1)
    centre(8)
    rows_in(8)
    first_pass(g_buf, zpg.at[1], 2 * x_lo)
    for h in range(4):
        spectra_b(1, x_lo, h)
    centre(4)
    rows_in(4)
    first_pass(m_buf, zm, 3 - 2 * x_lo)
    pairs(1, x_lo, b_done=True)
    centre(9)
    rows_in(9)
    first_pass(g_buf, zpg.at[1], 2 - 2 * x_lo)
    pairs(1, 1 - x_lo)

    lane = lax.broadcasted_iota(jnp.int32, (8, 128), 1)
    along = (lane - LAGS // 2).astype(F32)
    by_pair = sums[0]
    total = 1.0 + jnp.sum(by_pair, axis=1, keepdims=True)
    shift_r = jnp.sum(sums[1], axis=1, keepdims=True) / total
    shift_c = jnp.sum(by_pair * along, axis=1, keepdims=True) / total

    lane1 = lax.broadcasted_iota(jnp.int32, (1, 128), 1)
    guest_s = 3 - 2 * (gz + x_lo - 2 * gz * x_lo)
    for i in range(2):
        line = jnp.zeros((1, 128), F32)
        for t in range(2):
            s = 2 * gz if t == 0 else guest_s
            c_tile = 2 * z + (x_lo if t == 0 else 1 - x_lo)
            held = prior_own[0] if t == 0 else prior_guest[...]
            for j in range(2):
                n = t * 4 + i * 2 + j
                r = i * 2 + j
                place = s * 16 + 2 * c_tile + j
                flow_r = held[r : r + 1, :].astype(F32) + shift_r[n : n + 1, :]
                flow_c = held[4 + r : 5 + r, :].astype(F32) + shift_c[n : n + 1, :]
                line = line + jnp.where(lane1 == place, flow_r, 0.0) + jnp.where(lane1 == place + 64, flow_c, 0.0)
        flow_send[i : i + 1, :] = line

    n_all = n_gz * n_row * n_col
    me = (gz * n_row + row) * n_col + col
    for dg in range(n_gz):
        for dr in range(n_row):
            for dc in range(n_col):
                if dg or dr or dc:
                    pltpu.make_async_remote_copy(
                        src_ref=flow_send, dst_ref=flow_recv.at[me], send_sem=send_f, recv_sem=recv_f,
                        device_id=at(dg, dr, dc), device_id_type=MESH,
                    ).start()
    want = [row_order[2 * row + m] for m in range(2)]
    picked = [jnp.zeros((1, 128), F32) for _ in range(2)]
    others = flow_recv.at[pl.ds(0, n_all - 1)]
    pltpu.make_async_copy(others, others, recv_f).wait()
    flow_recv[pl.ds(me, 1)] = flow_send[...][None]
    for r in range(n_row):
        block = sum(jnp.sum(flow_recv[pl.ds((g * n_row + r) * n_col, n_col)], axis=0) for g in range(n_gz))
        for m in range(2):
            for i in range(2):
                hit = jnp.full((1, 128), want[m], jnp.int32) == 2 * r + i
                picked[m] = picked[m] + jnp.where(hit, block[i : i + 1, :], 0.0)
    for m in range(2):
        out[m : m + 1, :] = picked[m]
    pltpu.make_async_copy(others, others, send_f).wait()

    prior_send.wait_send()
    for k in range(12):
        def sent_all(k=k):
            for p in parts_of[k]:
                part(k, p, *sent[k]).wait_send()

        guarded(when_send, k, sent_all)

        def rows_sent(k=k):
            pl.when(has_up)(row_copy(k, 0).wait_send)
            pl.when(has_down)(row_copy(k, 1).wait_send)

        guarded(when_recv, k, rows_sent)


def body(sections, priors, row_order):
    table = forward_table()
    lag_cos, lag_sin = lag_tables()
    vmem = pl.BlockSpec(memory_space=pltpu.VMEM)
    dma = pltpu.SemaphoreType.DMA
    return pl.pallas_call(
        kernel,
        out_shape=jax.ShapeDtypeStruct((2, 128), F32),
        in_specs=[pl.BlockSpec(memory_space=pltpu.HBM)] * 8,
        out_specs=vmem,
        scratch_shapes=[
            pltpu.SMEM((2, 2, 2, 2), jnp.int32),
            pltpu.SMEM((16,), jnp.int32),
            pltpu.VMEM((512, 512), BF16),
            pltpu.VMEM((512, 512), BF16),
            pltpu.VMEM((LAGS, 512), F32),
            pltpu.VMEM((LAGS, 512), F32),
            pltpu.VMEM((8, 512), jnp.int32),
            pltpu.VMEM((768, 1280), BF16),
            pltpu.VMEM((2, 768, 768), BF16),
            pltpu.VMEM((2, 512, 1280), BF16),
            pltpu.VMEM((2, 2, 512, 768), BF16),
            pltpu.VMEM((2, 256, 512), F32),
            pltpu.VMEM((4, 256, 512), F32),
            pltpu.VMEM((2, 512, 512), BF16),
            pltpu.VMEM((2, 8, 128), jnp.int32),
            pltpu.VMEM((8, 128), jnp.int32),
            pltpu.VMEM((8, 512), F32),
            pltpu.VMEM((8, 512), F32),
            pltpu.VMEM((16, LAGS, 512), BF16),
            pltpu.VMEM((2, 8, 128), F32),
            pltpu.VMEM((2, 128), F32),
            pltpu.VMEM((128, 2, 128), F32),
            pltpu.SemaphoreType.REGULAR((4,)),
            dma((9,)),
            dma((37,)),
            dma((37,)),
            dma((24,)),
            dma((24,)),
            dma,
            dma,
        ],
        compiler_params=pltpu.CompilerParams(collective_id=0, has_side_effects=True, vmem_limit_bytes=67_043_328),
    )(
        sections, priors, row_order, jnp.asarray(table), jnp.asarray(np.ascontiguousarray(table.T)),
        jnp.asarray(lag_cos), jnp.asarray(lag_sin), jnp.asarray(phase_rows()),
    )


def solution(mesh):
    return jax.shard_map(
        body,
        mesh=mesh,
        in_specs=(P("gz", "row", "col"), P(None, "gz", "row", "col"), P()),
        out_specs=P("row", None),
        check_vma=False,
    )
```

```python
import functools

import jax
import jax.numpy as jnp
import ml_dtypes
import numpy as np
from jax import lax
from jax.experimental import pallas as pl
from jax.experimental.pallas import tpu as pltpu
from jax.sharding import PartitionSpec as P

PATCH = 512
LAGS = 128
UNIT = 128
MESH = pl.DeviceIdType.MESH
BF16 = jnp.bfloat16
F32 = jnp.float32


def slots():
    m = np.arange(128)
    freq = np.concatenate([2 * m, 2 * m, 2 * m + 1, 2 * m + 1])
    sine = np.concatenate([np.zeros(128), np.ones(128), np.zeros(128), np.ones(128)]).astype(bool)
    weight = np.full(512, 2.0)
    freq[128], sine[128] = 256, False
    weight[0] = weight[128] = 1.0
    return freq, sine, weight


def forward_table():
    freq, sine, _ = slots()
    angle = (freq[:, None] * np.arange(PATCH)[None, :]) % PATCH * (2.0 * np.pi / PATCH)
    return np.where(sine[:, None], np.sin(angle), np.cos(angle)).astype(ml_dtypes.bfloat16)


def lag_tables():
    freq, _, weight = slots()
    lag = np.arange(LAGS) - LAGS // 2
    angle = (freq[None, :] * lag[:, None]) % PATCH * (2.0 * np.pi / PATCH)
    return (np.cos(angle) * weight).astype(np.float32), (np.sin(angle) * weight).astype(np.float32)


def phase_rows():
    freq, sine, _ = slots()
    rows = np.zeros((8, 512), np.int32)
    rows[0] = freq
    rows[1] = np.where(sine, -128, 0)
    rows[2] = np.where(sine, 0, 128)
    rows[3] = 1
    rows[3, 128] = 0
    return rows


def cross_chunk(a, b, m_ref, kb, lb, rc):
    lc, ls = pl.ds(lb * 256, 128), pl.ds(lb * 256 + 128, 128)
    rt, rl = pl.ds(rc * 16, 16), pl.ds(128 + rc * 16, 16)
    mt, ml = pl.ds(kb * 256 + rc * 16, 16), pl.ds(kb * 256 + 128 + rc * 16, 16)
    a1, a2, a3, a4 = a[rt, lc], a[rt, ls], a[rl, lc], a[rl, ls]
    b1, b2, b3, b4 = b[rt, lc], b[rt, ls], b[rl, lc], b[rl, ls]
    p33, p44 = a3 * b3, a4 * b4
    u1, u2 = a1 * b2 - a2 * b1, a3 * b4 - a4 * b3
    v1, v2 = a1 * b3 - a3 * b1, a2 * b4 - a4 * b2
    ss = (a1 * b4 + a4 * b1) - (a2 * b3 + a3 * b2)
    first_row = kb == 0 and rc == 0
    if first_row:
        k0 = lax.broadcasted_iota(jnp.int32, (16, 128), 0) == 0
        z33, z44, zu2 = jnp.where(k0, 0.0, p33), jnp.where(k0, 0.0, p44), jnp.where(k0, 0.0, u2)
    else:
        z33, z44, zu2 = p33, p44, u2
    t1, t2 = a1 * b1 + z33, a2 * b2 + z44
    cc, cs, sc = t1 + t2, u1 + zu2, v1 + v2
    if first_row:
        sc, ss = jnp.where(k0, p33 + p44, sc), jnp.where(k0, u2, ss)
    if lb == 0:
        l0 = lax.broadcasted_iota(jnp.int32, (16, 128), 1) == 0
        cc, cs = jnp.where(l0, t1, cc), jnp.where(l0, t2, cs)
        if first_row:
            sc = jnp.where(l0, jnp.where(k0, p33, v1), sc)
            ss = jnp.where(l0, jnp.where(k0, p44, v2), ss)
        else:
            sc, ss = jnp.where(l0, v1, sc), jnp.where(l0, v2, ss)
    m_ref[mt, lc] = cc.astype(BF16)
    m_ref[mt, ls] = cs.astype(BF16)
    m_ref[ml, lc] = sc.astype(BF16)
    m_ref[ml, ls] = ss.astype(BF16)


def kernel(
    sections, priors_h, row_order_h, table_h, table_t_h, lag_cos_h, lag_sin_h, phases_h, out,
    priors, row_order, table, table_t, lag_cos, lag_sin, phases, m_buf, pg_buf, zm, zpg, a_s, b_s, mix, prior_own, prior_guest, u_s, v_s, lag_s, sums, flow_send, flow_recv, known,
    local_sem, send_x, recv_x, send_r, recv_r, send_f, recv_f,
):
    gz, row, col = lax.axis_index("gz"), lax.axis_index("row"), lax.axis_index("col")
    n_gz, n_row, n_col = lax.axis_size("gz"), lax.axis_size("row"), lax.axis_size("col")
    x_lo = lax.rem(col, 2)
    z = lax.div(col, 2)
    has_left, has_right = z > 0, z < n_col // 2 - 1
    has_out = jnp.logical_or(jnp.logical_and(x_lo == 0, has_left), jnp.logical_and(x_lo == 1, has_right))
    has_in = jnp.logical_or(jnp.logical_and(x_lo == 1, has_left), jnp.logical_and(x_lo == 0, has_right))
    has_up, has_down = row > 0, row < n_row - 1
    side = 2 * x_lo - 1
    a_id = (gz, row, col - side)
    b_id = (1 - gz, row, col - side)
    n_id = (gz, row, col + side)
    z_out = (gz, row, col + 2 * side)
    z_in = (gz, row, col - 2 * side)
    up_id, down_id = (gz, row - 1, col), (gz, row + 1, col)

    def al(v):
        return pl.multiple_of(v, 128)

    c0 = al(128 + 512 * x_lo)
    near, outer = al(512 + 128 * x_lo), al(128 + 896 * x_lo)
    near_p, outer_p = al(512 - 384 * x_lo), al(128 + 384 * x_lo)
    c1 = al(640 - 512 * x_lo)
    near_g, outer_g = al(640 - 128 * x_lo), al(1024 - 896 * x_lo)
    m_far_out, m_far_in = al(1152 * x_lo), al(1152 - 1152 * x_lo)
    side_in, side_out = al(640 - 640 * x_lo), al(640 * x_lo)
    body = pl.ds(128, 512)
    p_buf, g_buf = pg_buf.at[0], pg_buf.at[1]

    own_m = pltpu.make_async_copy(sections.at[x_lo], m_buf.at[body, pl.ds(c0, 512)], local_sem.at[0])
    own_p = pltpu.make_async_copy(sections.at[1 - x_lo], p_buf.at[body, pl.ds(128, 512)], local_sem.at[1])
    own_m.start()
    own_p.start()
    constants = [
        pltpu.make_async_copy(src, dst, local_sem.at[2 + k])
        for k, (src, dst) in enumerate([
            (priors_h, priors), (phases_h, phases), (table_h, table), (table_t_h, table_t),
            (lag_cos_h, lag_cos), (lag_sin_h, lag_sin), (row_order_h, row_order),
        ])
    ]
    for copy in constants:
        copy.start()

    def at(dg, dr, dc):
        return (lax.rem(gz + dg, n_gz), lax.rem(row + dr, n_row), lax.rem(col + dc, n_col))

    z_ring = [at(0, 0, 2), at(0, 0, n_col - 2)]
    row_ring = [at(0, 1, 0), at(0, n_row - 1, 0)]
    near_peers = [a_id, b_id] + z_ring + row_ring
    barrier = pltpu.get_barrier_semaphore()
    for peer in near_peers:
        pl.semaphore_signal(barrier, inc=1, device_id=peer, device_id_type=MESH)

    rounds = [
        near_peers,
        [a_id, b_id, (1 - gz, row, col)],
        z_ring + [at(0, 0, n_col // 2)],
        [at(0, 2, 0), at(0, n_row - 2, 0)],
    ]

    def tell(k):
        for peer in rounds[k]:
            pl.semaphore_signal(known.at[k], inc=1, device_id=peer, device_id_type=MESH)

    def hear(k):
        pl.semaphore_wait(known.at[k], len(rounds[k]))

    constants[0].wait()
    for c in range(2):
        for ii in range(2):
            for jj in range(2):
                r = c * 4 + ii * 2 + jj
                prior_own[0, r : r + 1, :] = jnp.full((1, 128), priors[c, 0, ii, jj], jnp.int32)
                prior_own[1, r : r + 1, :] = jnp.full((1, 128), priors[c, 1, ii, jj], jnp.int32)

    @pl.when(row == 0)
    def _():
        m_buf[0:128, :] = jnp.zeros((128, 1280), BF16)
        pg_buf[:, 0:128, :] = jnp.zeros((2, 128, 768), BF16)

    @pl.when(row == n_row - 1)
    def _():
        m_buf[640:768, :] = jnp.zeros((128, 1280), BF16)
        pg_buf[:, 640:768, :] = jnp.zeros((2, 128, 768), BF16)

    @pl.when(jnp.logical_not(has_left))
    def _():
        m_buf[:, 0:128] = jnp.zeros((768, 128), BF16)
        pg_buf[x_lo, :, 0:128] = jnp.zeros((768, 128), BF16)

    @pl.when(jnp.logical_not(has_right))
    def _():
        m_buf[:, 1152:1280] = jnp.zeros((768, 128), BF16)
        pg_buf[1 - x_lo, :, 640:768] = jnp.zeros((768, 128), BF16)

    own_m.wait()
    own_p.wait()
    pl.semaphore_wait(barrier, len(near_peers))
    tell(0)

    spans = (pl.ds(128, 128), pl.ds(512, 128), pl.ds(256, 256))

    def part(k, p, src, src_at, dst, dst_at, width, device):
        return pltpu.make_async_remote_copy(
            src_ref=src.at[spans[p], pl.ds(src_at, width)], dst_ref=dst.at[spans[p], pl.ds(dst_at, width)],
            send_sem=send_x.at[3 * k + p], recv_sem=recv_x.at[3 * k + p], device_id=device, device_id_type=MESH,
        )

    sent = {
        0: (p_buf, outer_p, m_buf, outer, 128, a_id),
        1: (p_buf, near_p, m_buf, near, 128, a_id),
        2: (m_buf, near, p_buf, side_out, 128, a_id),
        3: (m_buf, outer, p_buf, side_in, 128, n_id),
        4: (p_buf, 256, m_buf, al(c0 + 128), 256, a_id),
        5: (m_buf, outer, m_buf, m_far_in, 128, z_out),
        6: (m_buf, c0, g_buf, 128, 512, b_id),
        7: (m_buf, outer_g, m_buf, m_far_out, 128, z_in),
        8: (m_buf, near_g, g_buf, side_in, 128, b_id),
        9: (m_buf, m_far_out, g_buf, side_out, 128, b_id),
        10: (m_buf, c0, g_buf, 128, 256, b_id),
        11: (m_buf, al(c0 + 256), g_buf, 384, 256, b_id),
    }
    landed = {
        0: (m_buf, outer_g, 128), 1: (m_buf, near_g, 128), 2: (p_buf, side_in, 128), 3: (p_buf, side_out, 128),
        4: (m_buf, al(c1 + 128), 256), 5: (m_buf, m_far_in, 128), 6: (g_buf, 128, 512), 7: (m_buf, m_far_out, 128),
        8: (g_buf, side_out, 128), 9: (g_buf, side_in, 128), 10: (g_buf, 128, 256), 11: (g_buf, 384, 256),
    }
    parts_of = {k: (0, 1, 2) for k in range(10)}
    parts_of.update({6: (0, 1), 10: (2,), 11: (2,)})
    when_send = {3: has_out, 5: has_out, 7: has_in, 9: has_out}
    when_recv = {3: has_out, 5: has_in, 7: has_out, 9: has_in}

    def guarded(conds, k, do):
        if k in conds:
            pl.when(conds[k])(do)
        else:
            do()

    def send(k, *parts):
        def do():
            for p in parts:
                part(k, p, *sent[k]).start()

        guarded(when_send, k, do)

    def land(k, p):
        ref, start, width = landed[k]
        part(k, p, ref, start, ref, start, width, a_id).wait_recv()

    pieces = dict(landed)
    pieces.update({10: (m_buf, c0, 512), 11: (p_buf, 128, 512)})

    def row_copy(k, down):
        ref, start, width = pieces[k]
        cols = pl.ds(start, width)
        src, dst = (pl.ds(512, 128), pl.ds(0, 128)) if down else (pl.ds(128, 128), pl.ds(640, 128))
        return pltpu.make_async_remote_copy(
            src_ref=ref.at[src, cols], dst_ref=ref.at[dst, cols], send_sem=send_r.at[2 * k + down],
            recv_sem=recv_r.at[2 * k + down], device_id=down_id if down else up_id, device_id_type=MESH,
        )

    def send_row(k, down):
        pl.when(has_down if down else has_up)(row_copy(k, down).start)

    def edges(k, forward=None):
        def do():
            for p in range(2):
                land(k, p)
                send_row(k, p)

        guarded(when_recv, k, do)
        if forward is not None:
            send(forward, 0, 1)

    def centre(k, forward=None):
        guarded(when_recv, k, lambda: land(k, 2))
        if forward is not None:
            send(forward, 2)

    def rows_in(*ks):
        def do(k):
            pl.when(has_down)(row_copy(k, 0).wait_recv)
            pl.when(has_up)(row_copy(k, 1).wait_recv)

        for k in ks:
            guarded(when_recv, k, functools.partial(do, k))

    prior_id = (gz + x_lo * (1 - 2 * gz), row, col - side)
    prior_send = pltpu.make_async_remote_copy(
        src_ref=prior_own.at[1], dst_ref=prior_guest, send_sem=send_x.at[36], recv_sem=recv_x.at[36],
        device_id=prior_id, device_id_type=MESH,
    )

    prior_send.start()
    send(0, 0, 1)
    send(6, 0, 1)
    send(5, 0, 1)
    send(1, 0, 1)
    send(2, 0, 1)
    send(5, 2)
    send(1, 2)
    send(2, 2)
    send(0, 2)
    send(10, 2)
    for k in (10, 11):
        for down in range(2):
            send_row(k, down)

    for copy in constants[1:]:
        copy.wait()
    freq, off_u, off_v, mask_v = phases[0:1, :], phases[1:2, :], phases[2:3, :], phases[3:4, :]

    def lag_tables_of(t):
        value = prior_own[0] if t == 0 else prior_guest[...]
        sign = (1 - 2 * x_lo) * (1 - 2 * t)
        turn = jnp.concatenate([value] * 4, axis=1) * sign * freq
        scale = 2.0 * np.pi / PATCH
        u_s[...] = jnp.cos(((turn + off_u) & (PATCH - 1)).astype(F32) * scale)
        v_s[...] = jnp.cos(((turn + off_v) & (PATCH - 1)).astype(F32) * scale) * mask_v.astype(F32) * sign.astype(F32)

        @pl.loop(0, 8)
        def _(r):
            lag_s[8 * t + r] = (lag_cos[...] * u_s[pl.ds(r, 1), :] + lag_sin[...] * v_s[pl.ds(r, 1), :]).astype(BF16)

    reach = (lax.broadcasted_iota(jnp.int32, (LAGS, LAGS), 0) - LAGS // 2).astype(F32)
    unit = 1.0 / (512.0 * 512.0 * 512.0)

    def first_pass(src, dst, block):
        at = al(block * 256)
        for i in range(2):
            dst[i, :, pl.ds(at, 256)] = jnp.dot(
                table[...], src[pl.ds(256 * i, 512), pl.ds(at, 256)], preferred_element_type=F32
            ).astype(BF16)

    def pairs(t, j, between=None, b_done=False):
        tile = x_lo if t == 0 else 1 - x_lo
        at_m = al((tile * 2 + j) * 256)

        def spectra(h):
            i, kb = h // 2, h % 2
            a_s[h % 2] = jnp.dot(zm[i, pl.ds(kb * 256, 256), pl.ds(at_m, 512)], table_t[...], preferred_element_type=F32)
            if not b_done:
                spectra_b(t, j, h)

        def products(h):
            for rc in range(8):
                for lb in range(2):
                    cross_chunk(a_s.at[h % 2], b_s.at[h], mix.at[h // 2], h % 2, lb, rc)

        def window(i):
            n = t * 4 + i * 2 + j
            half = jnp.dot(lag_s[8 * t + i * 2 + j], mix[i], preferred_element_type=F32).astype(BF16)
            surface = unit * lax.dot_general(
                half, lag_s[8 * t + 4 + i * 2 + j], (((1,), (1,)), ((), ())), preferred_element_type=F32
            )
            weights = surface * surface
            sums[0, pl.ds(n, 1), :] = jnp.sum(weights, axis=0, keepdims=True)
            sums[1, pl.ds(n, 1), :] = jnp.sum(weights * reach, axis=0, keepdims=True)

        spectra(0)
        spectra(1)
        products(0)
        spectra(2)
        products(1)
        if between is not None:
            between()
        spectra(3)
        window(0)
        products(2)
        products(3)
        window(1)

    def spectra_b(t, j, h):
        b_s[h] = jnp.dot(
            zpg[t, h // 2, pl.ds(h % 2 * 256, 256), pl.ds(al(j * 256), 512)], table_t[...], preferred_element_type=F32
        )

    hear(0)
    send(3, 0, 1, 2)
    send(4, 0, 1, 2)
    tell(1)
    lag_tables_of(0)
    rows_in(10)
    first_pass(m_buf, zm, 1 + 2 * x_lo)
    edges(0, 7)
    rows_in(11)
    first_pass(p_buf, zpg.at[0], 1)
    edges(5)
    edges(1, 8)
    prior_send.wait_recv()
    lag_tables_of(1)
    edges(2)
    edges(7, 9)
    send(11, 2)
    centre(5)
    centre(1, 8)
    rows_in(1)
    first_pass(m_buf, zm, 2)
    hear(1)
    tell(2)
    centre(2)
    rows_in(2)
    first_pass(p_buf, zpg.at[0], 2 - 2 * x_lo)

    def arrivals():
        centre(0, 7)
        edges(3)

    pairs(0, 1 - x_lo, arrivals)
    edges(6)
    rows_in(0, 5)
    first_pass(m_buf, zm, 4 - 4 * x_lo)
    hear(2)
    tell(3)
    centre(7, 9)
    rows_in(7)
    first_pass(m_buf, zm, 4 * x_lo)
    edges(8)
    edges(9)
    centre(3)
    rows_in(3)
    first_pass(p_buf, zpg.at[0], 2 * x_lo)
    pairs(0, x_lo, lambda: edges(4))
    hear(3)
    centre(10)
    centre(11)
    rows_in(6)
    first_pass(g_buf, zpg.at[1], 1)
    centre(8)
    rows_in(8)
    first_pass(g_buf, zpg.at[1], 2 * x_lo)
    for h in range(4):
        spectra_b(1, x_lo, h)
    centre(4)
    rows_in(4)
    first_pass(m_buf, zm, 3 - 2 * x_lo)
    pairs(1, x_lo, b_done=True)
    centre(9)
    rows_in(9)
    first_pass(g_buf, zpg.at[1], 2 - 2 * x_lo)
    pairs(1, 1 - x_lo)

    lane = lax.broadcasted_iota(jnp.int32, (8, 128), 1)
    along = (lane - LAGS // 2).astype(F32)
    by_pair = sums[0]
    total = 1.0 + jnp.sum(by_pair, axis=1, keepdims=True)
    shift_r = jnp.sum(sums[1], axis=1, keepdims=True) / total
    shift_c = jnp.sum(by_pair * along, axis=1, keepdims=True) / total

    lane1 = lax.broadcasted_iota(jnp.int32, (1, 128), 1)
    guest_s = 3 - 2 * (gz + x_lo - 2 * gz * x_lo)
    for i in range(2):
        line = jnp.zeros((1, 128), F32)
        for t in range(2):
            s = 2 * gz if t == 0 else guest_s
            c_tile = 2 * z + (x_lo if t == 0 else 1 - x_lo)
            held = prior_own[0] if t == 0 else prior_guest[...]
            for j in range(2):
                n = t * 4 + i * 2 + j
                r = i * 2 + j
                place = s * 16 + 2 * c_tile + j
                flow_r = held[r : r + 1, :].astype(F32) + shift_r[n : n + 1, :]
                flow_c = held[4 + r : 5 + r, :].astype(F32) + shift_c[n : n + 1, :]
                line = line + jnp.where(lane1 == place, flow_r, 0.0) + jnp.where(lane1 == place + 64, flow_c, 0.0)
        flow_send[i : i + 1, :] = line

    n_all = n_gz * n_row * n_col
    me = (gz * n_row + row) * n_col + col
    def hops(e):
        return 2 * e[0] + min(e[1], n_row - e[1]) / 2 + min(e[2], n_col - e[2]) / 2

    shifts = [(dg, dr, dc) for dg in range(n_gz) for dr in range(n_row) for dc in range(n_col) if dg or dr or dc]
    for shift in sorted(shifts, key=hops, reverse=True):
        pltpu.make_async_remote_copy(
            src_ref=flow_send, dst_ref=flow_recv.at[me], send_sem=send_f, recv_sem=recv_f,
            device_id=at(*shift), device_id_type=MESH,
        ).start()
    want = [row_order[2 * row + m] for m in range(2)]
    picked = [jnp.zeros((1, 128), F32) for _ in range(2)]
    others = flow_recv.at[pl.ds(0, n_all - 1)]
    pltpu.make_async_copy(others, others, recv_f).wait()
    flow_recv[pl.ds(me, 1)] = flow_send[...][None]
    for r in range(n_row):
        block = sum(jnp.sum(flow_recv[pl.ds((g * n_row + r) * n_col, n_col)], axis=0) for g in range(n_gz))
        for m in range(2):
            for i in range(2):
                hit = jnp.full((1, 128), want[m], jnp.int32) == 2 * r + i
                picked[m] = picked[m] + jnp.where(hit, block[i : i + 1, :], 0.0)
    for m in range(2):
        out[m : m + 1, :] = picked[m]
    pltpu.make_async_copy(others, others, send_f).wait()

    prior_send.wait_send()
    for k in range(12):
        def sent_all(k=k):
            for p in parts_of[k]:
                part(k, p, *sent[k]).wait_send()

        guarded(when_send, k, sent_all)

        def rows_sent(k=k):
            pl.when(has_up)(row_copy(k, 0).wait_send)
            pl.when(has_down)(row_copy(k, 1).wait_send)

        guarded(when_recv, k, rows_sent)


def body(sections, priors, row_order):
    table = forward_table()
    lag_cos, lag_sin = lag_tables()
    vmem = pl.BlockSpec(memory_space=pltpu.VMEM)
    dma = pltpu.SemaphoreType.DMA
    return pl.pallas_call(
        kernel,
        out_shape=jax.ShapeDtypeStruct((2, 128), F32),
        in_specs=[pl.BlockSpec(memory_space=pltpu.HBM)] * 8,
        out_specs=vmem,
        scratch_shapes=[
            pltpu.SMEM((2, 2, 2, 2), jnp.int32),
            pltpu.SMEM((16,), jnp.int32),
            pltpu.VMEM((512, 512), BF16),
            pltpu.VMEM((512, 512), BF16),
            pltpu.VMEM((LAGS, 512), F32),
            pltpu.VMEM((LAGS, 512), F32),
            pltpu.VMEM((8, 512), jnp.int32),
            pltpu.VMEM((768, 1280), BF16),
            pltpu.VMEM((2, 768, 768), BF16),
            pltpu.VMEM((2, 512, 1280), BF16),
            pltpu.VMEM((2, 2, 512, 768), BF16),
            pltpu.VMEM((2, 256, 512), F32),
            pltpu.VMEM((4, 256, 512), F32),
            pltpu.VMEM((2, 512, 512), BF16),
            pltpu.VMEM((2, 8, 128), jnp.int32),
            pltpu.VMEM((8, 128), jnp.int32),
            pltpu.VMEM((8, 512), F32),
            pltpu.VMEM((8, 512), F32),
            pltpu.VMEM((16, LAGS, 512), BF16),
            pltpu.VMEM((2, 8, 128), F32),
            pltpu.VMEM((2, 128), F32),
            pltpu.VMEM((128, 2, 128), F32),
            pltpu.SemaphoreType.REGULAR((4,)),
            dma((9,)),
            dma((37,)),
            dma((37,)),
            dma((24,)),
            dma((24,)),
            dma,
            dma,
        ],
        compiler_params=pltpu.CompilerParams(collective_id=0, has_side_effects=True, vmem_limit_bytes=67_043_328),
    )(
        sections, priors, row_order, jnp.asarray(table), jnp.asarray(np.ascontiguousarray(table.T)),
        jnp.asarray(lag_cos), jnp.asarray(lag_sin), jnp.asarray(phase_rows()),
    )


def solution(mesh):
    return jax.shard_map(
        body,
        mesh=mesh,
        in_specs=(P("gz", "row", "col"), P(None, "gz", "row", "col"), P()),
        out_specs=P("row", None),
        check_vma=False,
    )
```

```python
import functools

import jax
import jax.numpy as jnp
import ml_dtypes
import numpy as np
from jax import lax
from jax.experimental import pallas as pl
from jax.experimental.pallas import tpu as pltpu
from jax.sharding import PartitionSpec as P

PATCH = 512
LAGS = 128
UNIT = 128
MESH = pl.DeviceIdType.MESH
BF16 = jnp.bfloat16
F32 = jnp.float32


def slots():
    m = np.arange(128)
    freq = np.concatenate([2 * m, 2 * m, 2 * m + 1, 2 * m + 1])
    sine = np.concatenate([np.zeros(128), np.ones(128), np.zeros(128), np.ones(128)]).astype(bool)
    weight = np.full(512, 2.0)
    freq[128], sine[128] = 256, False
    weight[0] = weight[128] = 1.0
    return freq, sine, weight


def forward_table():
    freq, sine, _ = slots()
    angle = (freq[:, None] * np.arange(PATCH)[None, :]) % PATCH * (2.0 * np.pi / PATCH)
    return np.where(sine[:, None], np.sin(angle), np.cos(angle)).astype(ml_dtypes.bfloat16)


def lag_tables():
    freq, _, weight = slots()
    lag = np.arange(LAGS) - LAGS // 2
    angle = (freq[None, :] * lag[:, None]) % PATCH * (2.0 * np.pi / PATCH)
    return (np.cos(angle) * weight).astype(np.float32), (np.sin(angle) * weight).astype(np.float32)


def phase_rows():
    freq, sine, _ = slots()
    rows = np.zeros((8, 512), np.int32)
    rows[0] = freq
    rows[1] = np.where(sine, -128, 0)
    rows[2] = np.where(sine, 0, 128)
    rows[3] = 1
    rows[3, 128] = 0
    return rows


def cross_chunk(a, b, m_ref, kb, lb, rc):
    lc, ls = pl.ds(lb * 256, 128), pl.ds(lb * 256 + 128, 128)
    rt, rl = pl.ds(rc * 16, 16), pl.ds(128 + rc * 16, 16)
    mt, ml = pl.ds(kb * 256 + rc * 16, 16), pl.ds(kb * 256 + 128 + rc * 16, 16)
    a1, a2, a3, a4 = a[rt, lc], a[rt, ls], a[rl, lc], a[rl, ls]
    b1, b2, b3, b4 = b[rt, lc], b[rt, ls], b[rl, lc], b[rl, ls]
    p33, p44 = a3 * b3, a4 * b4
    u1, u2 = a1 * b2 - a2 * b1, a3 * b4 - a4 * b3
    v1, v2 = a1 * b3 - a3 * b1, a2 * b4 - a4 * b2
    ss = (a1 * b4 + a4 * b1) - (a2 * b3 + a3 * b2)
    first_row = kb == 0 and rc == 0
    if first_row:
        k0 = lax.broadcasted_iota(jnp.int32, (16, 128), 0) == 0
        z33, z44, zu2 = jnp.where(k0, 0.0, p33), jnp.where(k0, 0.0, p44), jnp.where(k0, 0.0, u2)
    else:
        z33, z44, zu2 = p33, p44, u2
    t1, t2 = a1 * b1 + z33, a2 * b2 + z44
    cc, cs, sc = t1 + t2, u1 + zu2, v1 + v2
    if first_row:
        sc, ss = jnp.where(k0, p33 + p44, sc), jnp.where(k0, u2, ss)
    if lb == 0:
        l0 = lax.broadcasted_iota(jnp.int32, (16, 128), 1) == 0
        cc, cs = jnp.where(l0, t1, cc), jnp.where(l0, t2, cs)
        if first_row:
            sc = jnp.where(l0, jnp.where(k0, p33, v1), sc)
            ss = jnp.where(l0, jnp.where(k0, p44, v2), ss)
        else:
            sc, ss = jnp.where(l0, v1, sc), jnp.where(l0, v2, ss)
    m_ref[mt, lc] = cc.astype(BF16)
    m_ref[mt, ls] = cs.astype(BF16)
    m_ref[ml, lc] = sc.astype(BF16)
    m_ref[ml, ls] = ss.astype(BF16)


def kernel(
    sections, priors_h, row_order_h, table_h, table_t_h, lag_cos_h, lag_sin_h, phases_h, out,
    priors, row_order, table, table_t, lag_cos, lag_sin, phases, m_buf, pg_buf, zm, zpg, a_s, b_s, mix, prior_own, prior_guest, u_s, v_s, lag_s, sums, flow_send, flow_recv, known,
    local_sem, send_x, recv_x, send_r, recv_r, send_f, recv_f,
):
    gz, row, col = lax.axis_index("gz"), lax.axis_index("row"), lax.axis_index("col")
    n_gz, n_row, n_col = lax.axis_size("gz"), lax.axis_size("row"), lax.axis_size("col")
    x_lo = lax.rem(col, 2)
    z = lax.div(col, 2)
    has_left, has_right = z > 0, z < n_col // 2 - 1
    has_out = jnp.logical_or(jnp.logical_and(x_lo == 0, has_left), jnp.logical_and(x_lo == 1, has_right))
    has_in = jnp.logical_or(jnp.logical_and(x_lo == 1, has_left), jnp.logical_and(x_lo == 0, has_right))
    has_up, has_down = row > 0, row < n_row - 1
    side = 2 * x_lo - 1
    a_id = (gz, row, col - side)
    b_id = (1 - gz, row, col - side)
    n_id = (gz, row, col + side)
    z_out = (gz, row, col + 2 * side)
    z_in = (gz, row, col - 2 * side)
    up_id, down_id = (gz, row - 1, col), (gz, row + 1, col)

    def al(v):
        return pl.multiple_of(v, 128)

    c0 = al(128 + 512 * x_lo)
    near, outer = al(512 + 128 * x_lo), al(128 + 896 * x_lo)
    near_p, outer_p = al(512 - 384 * x_lo), al(128 + 384 * x_lo)
    c1 = al(640 - 512 * x_lo)
    near_g, outer_g = al(640 - 128 * x_lo), al(1024 - 896 * x_lo)
    m_far_out, m_far_in = al(1152 * x_lo), al(1152 - 1152 * x_lo)
    side_in, side_out = al(640 - 640 * x_lo), al(640 * x_lo)
    body = pl.ds(128, 512)
    p_buf, g_buf = pg_buf.at[0], pg_buf.at[1]

    def at(dg, dr, dc):
        return (lax.rem(gz + dg, n_gz), lax.rem(row + dr, n_row), lax.rem(col + dc, n_col))

    z_ring = [at(0, 0, 2), at(0, 0, n_col - 2)]
    row_ring = [at(0, 1, 0), at(0, n_row - 1, 0)]
    near_peers = [a_id, b_id] + z_ring + row_ring
    barrier = pltpu.get_barrier_semaphore()
    for peer in near_peers:
        pl.semaphore_signal(barrier, inc=1, device_id=peer, device_id_type=MESH)

    own_m = pltpu.make_async_copy(sections.at[x_lo], m_buf.at[body, pl.ds(c0, 512)], local_sem.at[0])
    own_p = pltpu.make_async_copy(sections.at[1 - x_lo], p_buf.at[body, pl.ds(128, 512)], local_sem.at[1])
    own_m.start()
    own_p.start()
    constants = [
        pltpu.make_async_copy(src, dst, local_sem.at[2 + k])
        for k, (src, dst) in enumerate([
            (priors_h, priors), (phases_h, phases), (table_h, table), (table_t_h, table_t),
            (lag_cos_h, lag_cos), (lag_sin_h, lag_sin), (row_order_h, row_order),
        ])
    ]
    for copy in constants:
        copy.start()

    rounds = [
        near_peers,
        [a_id, b_id, (1 - gz, row, col)],
        z_ring + [at(0, 0, n_col // 2)],
        [at(0, 2, 0), at(0, n_row - 2, 0)],
    ]

    def tell(k):
        for peer in rounds[k]:
            pl.semaphore_signal(known.at[k], inc=1, device_id=peer, device_id_type=MESH)

    def hear(k):
        pl.semaphore_wait(known.at[k], len(rounds[k]))

    constants[0].wait()
    for c in range(2):
        for ii in range(2):
            for jj in range(2):
                r = c * 4 + ii * 2 + jj
                prior_own[0, r : r + 1, :] = jnp.full((1, 128), priors[c, 0, ii, jj], jnp.int32)
                prior_own[1, r : r + 1, :] = jnp.full((1, 128), priors[c, 1, ii, jj], jnp.int32)

    @pl.when(row == 0)
    def _():
        m_buf[0:128, :] = jnp.zeros((128, 1280), BF16)
        pg_buf[:, 0:128, :] = jnp.zeros((2, 128, 768), BF16)

    @pl.when(row == n_row - 1)
    def _():
        m_buf[640:768, :] = jnp.zeros((128, 1280), BF16)
        pg_buf[:, 640:768, :] = jnp.zeros((2, 128, 768), BF16)

    @pl.when(jnp.logical_not(has_left))
    def _():
        m_buf[:, 0:128] = jnp.zeros((768, 128), BF16)
        pg_buf[x_lo, :, 0:128] = jnp.zeros((768, 128), BF16)

    @pl.when(jnp.logical_not(has_right))
    def _():
        m_buf[:, 1152:1280] = jnp.zeros((768, 128), BF16)
        pg_buf[1 - x_lo, :, 640:768] = jnp.zeros((768, 128), BF16)

    own_m.wait()
    own_p.wait()
    pl.semaphore_wait(barrier, len(near_peers))
    tell(0)

    spans = (pl.ds(128, 128), pl.ds(512, 128), pl.ds(256, 256))

    def part(k, p, src, src_at, dst, dst_at, width, device):
        return pltpu.make_async_remote_copy(
            src_ref=src.at[spans[p], pl.ds(src_at, width)], dst_ref=dst.at[spans[p], pl.ds(dst_at, width)],
            send_sem=send_x.at[3 * k + p], recv_sem=recv_x.at[3 * k + p], device_id=device, device_id_type=MESH,
        )

    sent = {
        0: (p_buf, outer_p, m_buf, outer, 128, a_id),
        1: (p_buf, near_p, m_buf, near, 128, a_id),
        2: (m_buf, near, p_buf, side_out, 128, a_id),
        3: (m_buf, outer, p_buf, side_in, 128, n_id),
        4: (p_buf, 256, m_buf, al(c0 + 128), 256, a_id),
        5: (m_buf, outer, m_buf, m_far_in, 128, z_out),
        6: (m_buf, c0, g_buf, 128, 512, b_id),
        7: (m_buf, outer_g, m_buf, m_far_out, 128, z_in),
        8: (m_buf, near_g, g_buf, side_in, 128, b_id),
        9: (m_buf, m_far_out, g_buf, side_out, 128, b_id),
        10: (m_buf, c0, g_buf, 128, 256, b_id),
        11: (m_buf, al(c0 + 256), g_buf, 384, 256, b_id),
    }
    landed = {
        0: (m_buf, outer_g, 128), 1: (m_buf, near_g, 128), 2: (p_buf, side_in, 128), 3: (p_buf, side_out, 128),
        4: (m_buf, al(c1 + 128), 256), 5: (m_buf, m_far_in, 128), 6: (g_buf, 128, 512), 7: (m_buf, m_far_out, 128),
        8: (g_buf, side_out, 128), 9: (g_buf, side_in, 128), 10: (g_buf, 128, 256), 11: (g_buf, 384, 256),
    }
    parts_of = {k: (0, 1, 2) for k in range(10)}
    parts_of.update({6: (0, 1), 10: (2,), 11: (2,)})
    when_send = {3: has_out, 5: has_out, 7: has_in, 9: has_out}
    when_recv = {3: has_out, 5: has_in, 7: has_out, 9: has_in}

    def guarded(conds, k, do):
        if k in conds:
            pl.when(conds[k])(do)
        else:
            do()

    def send(k, *parts):
        def do():
            for p in parts:
                part(k, p, *sent[k]).start()

        guarded(when_send, k, do)

    def land(k, p):
        ref, start, width = landed[k]
        part(k, p, ref, start, ref, start, width, a_id).wait_recv()

    pieces = dict(landed)
    pieces.update({10: (m_buf, c0, 512), 11: (p_buf, 128, 512)})

    def row_copy(k, down):
        ref, start, width = pieces[k]
        cols = pl.ds(start, width)
        src, dst = (pl.ds(512, 128), pl.ds(0, 128)) if down else (pl.ds(128, 128), pl.ds(640, 128))
        return pltpu.make_async_remote_copy(
            src_ref=ref.at[src, cols], dst_ref=ref.at[dst, cols], send_sem=send_r.at[2 * k + down],
            recv_sem=recv_r.at[2 * k + down], device_id=down_id if down else up_id, device_id_type=MESH,
        )

    def send_row(k, down):
        pl.when(has_down if down else has_up)(row_copy(k, down).start)

    def edges(k, forward=None):
        def do():
            for p in range(2):
                land(k, p)
                send_row(k, p)

        guarded(when_recv, k, do)
        if forward is not None:
            send(forward, 0, 1)

    def centre(k, forward=None):
        guarded(when_recv, k, lambda: land(k, 2))
        if forward is not None:
            send(forward, 2)

    def rows_in(*ks):
        def do(k):
            pl.when(has_down)(row_copy(k, 0).wait_recv)
            pl.when(has_up)(row_copy(k, 1).wait_recv)

        for k in ks:
            guarded(when_recv, k, functools.partial(do, k))

    prior_id = (gz + x_lo * (1 - 2 * gz), row, col - side)
    prior_send = pltpu.make_async_remote_copy(
        src_ref=prior_own.at[1], dst_ref=prior_guest, send_sem=send_x.at[36], recv_sem=recv_x.at[36],
        device_id=prior_id, device_id_type=MESH,
    )

    prior_send.start()
    send(0, 0, 1)
    send(6, 0, 1)
    send(5, 0, 1)
    send(1, 0, 1)
    send(2, 0, 1)
    send(5, 2)
    send(1, 2)
    send(2, 2)
    send(0, 2)
    for k in (10, 11):
        for down in range(2):
            send_row(k, down)

    for copy in constants[1:]:
        copy.wait()
    freq, off_u, off_v, mask_v = phases[0:1, :], phases[1:2, :], phases[2:3, :], phases[3:4, :]

    def lag_tables_of(t):
        value = prior_own[0] if t == 0 else prior_guest[...]
        sign = (1 - 2 * x_lo) * (1 - 2 * t)
        turn = jnp.concatenate([value] * 4, axis=1) * sign * freq
        scale = 2.0 * np.pi / PATCH
        u_s[...] = jnp.cos(((turn + off_u) & (PATCH - 1)).astype(F32) * scale)
        v_s[...] = jnp.cos(((turn + off_v) & (PATCH - 1)).astype(F32) * scale) * mask_v.astype(F32) * sign.astype(F32)

        @pl.loop(0, 8)
        def _(r):
            lag_s[8 * t + r] = (lag_cos[...] * u_s[pl.ds(r, 1), :] + lag_sin[...] * v_s[pl.ds(r, 1), :]).astype(BF16)

    reach = (lax.broadcasted_iota(jnp.int32, (LAGS, LAGS), 0) - LAGS // 2).astype(F32)
    unit = 1.0 / (512.0 * 512.0 * 512.0)

    def first_pass(src, dst, block):
        at = al(block * 256)
        for i in range(2):
            dst[i, :, pl.ds(at, 256)] = jnp.dot(
                table[...], src[pl.ds(256 * i, 512), pl.ds(at, 256)], preferred_element_type=F32
            ).astype(BF16)

    def pairs(t, j, between=None, b_done=False):
        tile = x_lo if t == 0 else 1 - x_lo
        at_m = al((tile * 2 + j) * 256)

        def spectra(h):
            i, kb = h // 2, h % 2
            a_s[h % 2] = jnp.dot(zm[i, pl.ds(kb * 256, 256), pl.ds(at_m, 512)], table_t[...], preferred_element_type=F32)
            if not b_done:
                spectra_b(t, j, h)

        def products(h):
            for rc in range(8):
                for lb in range(2):
                    cross_chunk(a_s.at[h % 2], b_s.at[h], mix.at[h // 2], h % 2, lb, rc)

        def window(i):
            n = t * 4 + i * 2 + j
            half = jnp.dot(lag_s[8 * t + i * 2 + j], mix[i], preferred_element_type=F32).astype(BF16)
            surface = unit * lax.dot_general(
                half, lag_s[8 * t + 4 + i * 2 + j], (((1,), (1,)), ((), ())), preferred_element_type=F32
            )
            weights = surface * surface
            sums[0, pl.ds(n, 1), :] = jnp.sum(weights, axis=0, keepdims=True)
            sums[1, pl.ds(n, 1), :] = jnp.sum(weights * reach, axis=0, keepdims=True)

        spectra(0)
        spectra(1)
        products(0)
        spectra(2)
        products(1)
        if between is not None:
            between()
        spectra(3)
        window(0)
        products(2)
        products(3)
        window(1)

    def spectra_b(t, j, h):
        b_s[h] = jnp.dot(
            zpg[t, h // 2, pl.ds(h % 2 * 256, 256), pl.ds(al(j * 256), 512)], table_t[...], preferred_element_type=F32
        )

    hear(0)
    send(3, 0, 1, 2)
    send(4, 0, 1, 2)
    tell(1)
    lag_tables_of(0)
    edges(0, 7)
    rows_in(10)
    first_pass(m_buf, zm, 1 + 2 * x_lo)
    edges(1, 8)
    send(10, 2)
    edges(2)
    edges(7, 9)
    send(11, 2)
    rows_in(11)
    first_pass(p_buf, zpg.at[0], 1)
    edges(5)
    prior_send.wait_recv()
    lag_tables_of(1)
    centre(5)
    centre(1, 8)
    rows_in(1)
    first_pass(m_buf, zm, 2)
    hear(1)
    tell(2)
    centre(2)
    rows_in(2)
    first_pass(p_buf, zpg.at[0], 2 - 2 * x_lo)

    def arrivals():
        centre(0, 7)
        edges(3)

    pairs(0, 1 - x_lo, arrivals)
    edges(6)
    rows_in(0, 5)
    first_pass(m_buf, zm, 4 - 4 * x_lo)
    hear(2)
    tell(3)
    centre(7, 9)
    rows_in(7)
    first_pass(m_buf, zm, 4 * x_lo)
    edges(8)
    edges(9)
    centre(3)
    rows_in(3)
    first_pass(p_buf, zpg.at[0], 2 * x_lo)
    pairs(0, x_lo, lambda: edges(4))
    hear(3)
    centre(10)
    centre(11)
    rows_in(6)
    first_pass(g_buf, zpg.at[1], 1)
    centre(8)
    rows_in(8)
    first_pass(g_buf, zpg.at[1], 2 * x_lo)
    for h in range(4):
        spectra_b(1, x_lo, h)
    centre(4)
    rows_in(4)
    first_pass(m_buf, zm, 3 - 2 * x_lo)
    pairs(1, x_lo, b_done=True)
    centre(9)
    rows_in(9)
    first_pass(g_buf, zpg.at[1], 2 - 2 * x_lo)
    pairs(1, 1 - x_lo)

    lane = lax.broadcasted_iota(jnp.int32, (8, 128), 1)
    along = (lane - LAGS // 2).astype(F32)
    by_pair = sums[0]
    total = 1.0 + jnp.sum(by_pair, axis=1, keepdims=True)
    shift_r = jnp.sum(sums[1], axis=1, keepdims=True) / total
    shift_c = jnp.sum(by_pair * along, axis=1, keepdims=True) / total

    lane1 = lax.broadcasted_iota(jnp.int32, (1, 128), 1)
    guest_s = 3 - 2 * (gz + x_lo - 2 * gz * x_lo)
    for i in range(2):
        line = jnp.zeros((1, 128), F32)
        for t in range(2):
            s = 2 * gz if t == 0 else guest_s
            c_tile = 2 * z + (x_lo if t == 0 else 1 - x_lo)
            held = prior_own[0] if t == 0 else prior_guest[...]
            for j in range(2):
                n = t * 4 + i * 2 + j
                r = i * 2 + j
                place = s * 16 + 2 * c_tile + j
                flow_r = held[r : r + 1, :].astype(F32) + shift_r[n : n + 1, :]
                flow_c = held[4 + r : 5 + r, :].astype(F32) + shift_c[n : n + 1, :]
                line = line + jnp.where(lane1 == place, flow_r, 0.0) + jnp.where(lane1 == place + 64, flow_c, 0.0)
        flow_send[i : i + 1, :] = line

    n_all = n_gz * n_row * n_col
    me = (gz * n_row + row) * n_col + col
    def hops(e):
        return 2 * e[0] + min(e[1], n_row - e[1]) / 2 + min(e[2], n_col - e[2]) / 2

    shifts = [(dg, dr, dc) for dg in range(n_gz) for dr in range(n_row) for dc in range(n_col) if dg or dr or dc]
    for shift in sorted(shifts, key=hops, reverse=True):
        pltpu.make_async_remote_copy(
            src_ref=flow_send, dst_ref=flow_recv.at[me], send_sem=send_f, recv_sem=recv_f,
            device_id=at(*shift), device_id_type=MESH,
        ).start()
    want = [row_order[2 * row + m] for m in range(2)]
    picked = [jnp.zeros((1, 128), F32) for _ in range(2)]
    others = flow_recv.at[pl.ds(0, n_all - 1)]
    pltpu.make_async_copy(others, others, recv_f).wait()
    flow_recv[pl.ds(me, 1)] = flow_send[...][None]
    for r in range(n_row):
        block = sum(jnp.sum(flow_recv[pl.ds((g * n_row + r) * n_col, n_col)], axis=0) for g in range(n_gz))
        for m in range(2):
            for i in range(2):
                hit = jnp.full((1, 128), want[m], jnp.int32) == 2 * r + i
                picked[m] = picked[m] + jnp.where(hit, block[i : i + 1, :], 0.0)
    for m in range(2):
        out[m : m + 1, :] = picked[m]
    pltpu.make_async_copy(others, others, send_f).wait()

    prior_send.wait_send()
    for k in range(12):
        def sent_all(k=k):
            for p in parts_of[k]:
                part(k, p, *sent[k]).wait_send()

        guarded(when_send, k, sent_all)

        def rows_sent(k=k):
            pl.when(has_up)(row_copy(k, 0).wait_send)
            pl.when(has_down)(row_copy(k, 1).wait_send)

        guarded(when_recv, k, rows_sent)


def body(sections, priors, row_order):
    table = forward_table()
    lag_cos, lag_sin = lag_tables()
    vmem = pl.BlockSpec(memory_space=pltpu.VMEM)
    dma = pltpu.SemaphoreType.DMA
    return pl.pallas_call(
        kernel,
        out_shape=jax.ShapeDtypeStruct((2, 128), F32),
        in_specs=[pl.BlockSpec(memory_space=pltpu.HBM)] * 8,
        out_specs=vmem,
        scratch_shapes=[
            pltpu.SMEM((2, 2, 2, 2), jnp.int32),
            pltpu.SMEM((16,), jnp.int32),
            pltpu.VMEM((512, 512), BF16),
            pltpu.VMEM((512, 512), BF16),
            pltpu.VMEM((LAGS, 512), F32),
            pltpu.VMEM((LAGS, 512), F32),
            pltpu.VMEM((8, 512), jnp.int32),
            pltpu.VMEM((768, 1280), BF16),
            pltpu.VMEM((2, 768, 768), BF16),
            pltpu.VMEM((2, 512, 1280), BF16),
            pltpu.VMEM((2, 2, 512, 768), BF16),
            pltpu.VMEM((2, 256, 512), F32),
            pltpu.VMEM((4, 256, 512), F32),
            pltpu.VMEM((2, 512, 512), BF16),
            pltpu.VMEM((2, 8, 128), jnp.int32),
            pltpu.VMEM((8, 128), jnp.int32),
            pltpu.VMEM((8, 512), F32),
            pltpu.VMEM((8, 512), F32),
            pltpu.VMEM((16, LAGS, 512), BF16),
            pltpu.VMEM((2, 8, 128), F32),
            pltpu.VMEM((2, 128), F32),
            pltpu.VMEM((128, 2, 128), F32),
            pltpu.SemaphoreType.REGULAR((4,)),
            dma((9,)),
            dma((37,)),
            dma((37,)),
            dma((24,)),
            dma((24,)),
            dma,
            dma,
        ],
        compiler_params=pltpu.CompilerParams(collective_id=0, has_side_effects=True, vmem_limit_bytes=67_043_328),
    )(
        sections, priors, row_order, jnp.asarray(table), jnp.asarray(np.ascontiguousarray(table.T)),
        jnp.asarray(lag_cos), jnp.asarray(lag_sin), jnp.asarray(phase_rows()),
    )


def solution(mesh):
    return jax.shard_map(
        body,
        mesh=mesh,
        in_specs=(P("gz", "row", "col"), P(None, "gz", "row", "col"), P()),
        out_specs=P("row", None),
        check_vma=False,
    )
```
